128 devices in a mesh: row: 16 (over x, y), col: 8 (over z, core).
Axes of the slice: x: 4, y: 4, z: 4, core: 2. Of those that a mesh axis runs over, the one named last changes fastest.
Arguments:
- signal: float32 [256, 256, 16, 256], P('row', 'col'), may hold values from -40 to 40, as said below
- start_frames: float32 [256, 32], replicated, may hold values from -6 to 6
- start_sends: float32 [16, 8], replicated, may hold values from -6 to 6
- start_rows: float32 [256, 64], replicated, may hold values from -6 to 6
- start_cols: float32 [256, 64], replicated, may hold values from -6 to 6
- rank_frames: int32 [1], replicated, may hold values from 16 to 32
- rank_sends: int32 [1], replicated, may hold values from 4 to 8
Outputs:
- filtered: float32 [256, 256, 16, 256], P('row', 'col')
The draws below stay inside these ranges and needn't reach their ends.
Inputs may be any that keep to these rules, and one draw needn't show every extreme that they name: `signal`: beamformed samples.
All inputs are finite; a program needn't handle non-finite values.
Results may differ from the reference program's by a relative error of at most 0.0003.
Values sent between devices are 32-bit elements; how exact they have to be, the bound alone decides.
A program may use at most 128 MiB of HBM per device.

```python
import math
import jax
import jax.numpy as jnp
from jax import lax

NT = 256
NK = 16
TMAX = 32
KMAX = 8
RS = 64
ITERS = 2
CORE_W = 256
NR = 256
NC = 256


def cosine_modes(length):
    places = jnp.arange(length, dtype=jnp.float32)
    return jnp.cos(math.pi * (places[:, None] + 0.5) * places[None, :] / length) * math.sqrt(2.0 / length)


def slow_waves(key, length, count, first):
    places = jnp.arange(length, dtype=jnp.float32)
    phases = jax.random.uniform(key, (count,), jnp.float32, -math.pi, math.pi)
    freqs = jnp.arange(count, dtype=jnp.float32) + first
    return jnp.cos(2.0 * math.pi * places[:, None] * freqs[None, :] / length + phases[None, :]) * math.sqrt(2.0)


def draw_signal(key, part):
    keys = jax.random.split(jax.random.fold_in(key, 7331), 8)
    maps_count = 64
    row_modes = cosine_modes(NR)
    col_modes = cosine_modes(NC)
    row_decay = jnp.exp(-4.0 * jnp.arange(NR, dtype=jnp.float32) / NR)
    col_decay = jnp.exp(-4.0 * jnp.arange(NC, dtype=jnp.float32) / NC)
    coeffs = jax.random.normal(keys[0], (maps_count, NR, NC), jnp.float32)
    coeffs = coeffs * row_decay[None, :, None] * col_decay[None, None, :]
    half_maps = jnp.einsum('rj,qjc->qrc', row_modes, coeffs)
    maps = jnp.einsum('qrj,cj->qrc', half_maps, col_modes)
    frame_base = jnp.concatenate([slow_waves(keys[1], NT, 4, 1.0), jax.random.normal(keys[2], (NT, NT - 4), jnp.float32)], axis=1)
    frame_mix = frame_base * jnp.exp(-3.0 * jnp.arange(NT, dtype=jnp.float32) / NT)[None, :]
    send_base = jnp.concatenate([slow_waves(keys[3], NK, 2, 0.5), jax.random.normal(keys[4], (NK, NK - 2), jnp.float32)], axis=1)
    send_mix = send_base * jnp.exp(-2.0 * jnp.arange(NK, dtype=jnp.float32) / NK)[None, :]
    mixing = jax.random.normal(keys[5], (maps_count, NK, NT), jnp.float32)
    profiles = jnp.einsum('ka,qab,tb->qkt', send_mix, mixing, frame_mix)
    tissue = jnp.dot(maps.reshape(maps_count, -1).T, profiles.reshape(maps_count, -1))
    tissue = tissue.reshape(NR, NC, NK, NT)
    tissue = tissue * (4.0 / jnp.sqrt(jnp.mean(tissue * tissue)))
    noise = jax.random.truncated_normal(keys[7], -6.0, 6.0, (NR, NC, NK, NT), jnp.float32)
    signal = tissue + noise
    return jnp.clip(signal, -40.0, 40.0)


def scatter_about(key, shape, scale, bound, kind=jnp.bfloat16):
    drawn = jax.random.normal(key, shape, jnp.float32) * scale
    return jnp.minimum(jnp.maximum(drawn, -bound), bound).astype(kind)


def setup_inputs(seed: int = 0) -> dict:
    streams_of = jax.random.split(jax.random.key(seed), 8)
    signal = draw_signal(jax.random.fold_in(streams_of[7], 71), 0)
    start_frames = scatter_about(streams_of[1], (NT, TMAX), 1.0, 6.0, jnp.float32)
    start_sends = scatter_about(streams_of[2], (NK, KMAX), 1.0, 6.0, jnp.float32)
    start_rows = scatter_about(streams_of[3], (NR, RS), 1.0, 6.0, jnp.float32)
    start_cols = scatter_about(streams_of[4], (NC, RS), 1.0, 6.0, jnp.float32)
    rank_frames = jax.random.randint(streams_of[5], (1,), TMAX // 2, TMAX + 1).astype(jnp.int32)
    rank_sends = jax.random.randint(streams_of[6], (1,), KMAX // 2, KMAX + 1).astype(jnp.int32)
    return dict(signal=signal, start_frames=start_frames, start_sends=start_sends, start_rows=start_rows, start_cols=start_cols, rank_frames=rank_frames, rank_sends=rank_sends)


def orthonormal(gram, start):
    high = lax.Precision.HIGHEST
    basis = start
    for rounds in range(ITERS):
        image = jnp.dot(gram, basis, precision=high)
        inner = jnp.dot(image.T, image, precision=high)
        factor = jnp.linalg.cholesky(inner)
        basis = jax.scipy.linalg.solve_triangular(factor, image.T, lower=True).T
    return basis

def reference(signal, start_frames, start_sends, start_rows, start_cols, rank_frames, rank_sends):
    high = lax.Precision.HIGHEST
    total_rows, total_cols = (signal.shape[0], signal.shape[1])
    flattened = signal.reshape(-1, NT)
    blocks = signal.reshape(-1, NK, NT)
    gram_frames = jnp.dot(flattened.T, flattened, precision=high)
    gram_sends = jnp.einsum('pkt,pjt->kj', blocks, blocks, precision=high)
    keep_frames = (jnp.arange(TMAX, dtype=jnp.int32) < rank_frames[0]).astype(jnp.float32)
    keep_sends = (jnp.arange(KMAX, dtype=jnp.int32) < rank_sends[0]).astype(jnp.float32)
    basis_frames = orthonormal(gram_frames, start_frames) * keep_frames[None, :]
    basis_sends = orthonormal(gram_sends, start_sends) * keep_sends[None, :]
    reduced = jnp.dot(flattened, basis_frames, precision=high).reshape(-1, NK, TMAX)
    core = jnp.einsum('pkb,ka->pab', reduced, basis_sends, precision=high)
    unfolded = core.reshape(total_rows, -1)
    gram_rows = jnp.dot(unfolded, unfolded.T, precision=high)
    basis_rows = orthonormal(gram_rows, start_rows)
    second = jnp.dot(basis_rows.T, unfolded, precision=high).reshape(RS, total_cols, CORE_W)
    gram_cols = jnp.einsum('sce,sde->cd', second, second, precision=high)
    basis_cols = orthonormal(gram_cols, start_cols)
    third = jnp.einsum('cu,sce->sue', basis_cols, second, precision=high)
    back_cols = jnp.einsum('cu,sue->sce', basis_cols, third, precision=high)
    tissue_core = jnp.dot(basis_rows, back_cols.reshape(RS, -1), precision=high)
    tissue_core = tissue_core.reshape(-1, KMAX, TMAX)
    expanded = jnp.einsum('pab,ka->pkb', tissue_core, basis_sends, precision=high)
    tissue = jnp.dot(expanded.reshape(-1, TMAX), basis_frames.T, precision=high).reshape(signal.shape)
    return signal - tissue
```

```python
import functools

import jax
import jax.numpy as jnp
from jax import lax
from jax.experimental import pallas as pl
from jax.experimental.pallas import tpu as pltpu
from jax.sharding import PartitionSpec as P

NT = 256
NK = 16
TMAX = 32
KMAX = 8
RS = 64
ITERS = 2
CORE_W = 256
NDEV = 128
MESH = pl.DeviceIdType.MESH


def me_index():
    return lax.axis_index("row") * 8 + lax.axis_index("col")


def coords(dev):
    return (dev // 8, dev % 8)


def reduce_kernel(pieces, x_ref, g_ref, inbox, sem_out, sem_in, sem_out2, sem_in2):
    me = me_index()
    barrier = pltpu.get_barrier_semaphore()

    def greet(s, _):
        dev = (me + s) % NDEV
        pl.semaphore_signal(barrier, inc=1, device_id=coords(dev), device_id_type=MESH)
        return 0

    lax.fori_loop(1, NDEV, greet, 0)
    pl.semaphore_wait(barrier, NDEV - 1)

    chip = me // 2
    reducer = jnp.logical_and(me % 2 == 1, chip < pieces)
    first = chip % pieces

    def scatter(s, _):
        piece = (first + s) % pieces
        dev = 2 * piece + 1

        @pl.when(dev != me)
        def _():
            slot = (me - dev + 2 * NDEV - 1) % NDEV
            pltpu.make_async_remote_copy(
                src_ref=x_ref.at[piece],
                dst_ref=inbox.at[slot],
                send_sem=sem_out,
                recv_sem=sem_in,
                device_id=coords(dev),
                device_id_type=MESH,
            ).start()

        return 0

    lax.fori_loop(0, pieces, scatter, 0)

    @pl.when(reducer)
    def _():
        whole = inbox.at[pl.ds(0, NDEV - 1)]
        pltpu.make_async_copy(whole, whole, sem_in).wait()
        total = jnp.sum(inbox[...], axis=0) + x_ref[chip]
        g_ref[chip] = total

        def spread(s, _):
            dev = (me + s) % NDEV
            pltpu.make_async_remote_copy(
                src_ref=g_ref.at[chip],
                dst_ref=g_ref.at[chip],
                send_sem=sem_out2,
                recv_sem=sem_in2,
                device_id=coords(dev),
                device_id_type=MESH,
            ).start()
            return 0

        lax.fori_loop(1, NDEV, spread, 0)
        some = x_ref.at[pl.ds(0, pieces - 1)]
        pltpu.make_async_copy(some, some, sem_in2).wait()
        pltpu.make_async_copy(some, some, sem_out).wait()
        pltpu.make_async_copy(whole, whole, sem_out2).wait()

    @pl.when(jnp.logical_not(reducer))
    def _():
        every = x_ref.at[pl.ds(0, pieces)]
        pltpu.make_async_copy(every, every, sem_in2).wait()
        pltpu.make_async_copy(every, every, sem_out).wait()


def all_sum(tiles, ident):
    pieces = tiles.shape[0]
    return pl.pallas_call(
        functools.partial(reduce_kernel, pieces),
        out_shape=jax.ShapeDtypeStruct(tiles.shape, jnp.float32),
        in_specs=[pl.BlockSpec(memory_space=pltpu.VMEM)],
        out_specs=pl.BlockSpec(memory_space=pltpu.VMEM),
        scratch_shapes=[
            pltpu.VMEM((NDEV - 1, 8, 128), jnp.float32),
            pltpu.SemaphoreType.DMA,
            pltpu.SemaphoreType.DMA,
            pltpu.SemaphoreType.DMA,
            pltpu.SemaphoreType.DMA,
        ],
        compiler_params=pltpu.CompilerParams(collective_id=ident, has_side_effects=True),
        name=f"all_sum_{ident}",
    )(tiles)


def packed(gram):
    return jnp.concatenate(
        [gram[:128, :128].reshape(16, 8, 128), gram[:128, 128:].reshape(16, 8, 128), gram[128:, 128:].reshape(16, 8, 128)]
    )


def unpacked(tiles):
    a = tiles[:16].reshape(128, 128)
    b = tiles[16:32].reshape(128, 128)
    c = tiles[32:48].reshape(128, 128)
    return jnp.concatenate([jnp.concatenate([a, b], 1), jnp.concatenate([b.T, c], 1)], 0)


def orthonormal(gram, start):
    high = lax.Precision.HIGHEST
    basis = start
    for rounds in range(ITERS):
        image = jnp.dot(gram, basis, precision=high)
        inner = jnp.dot(image.T, image, precision=high)
        factor = jnp.linalg.cholesky(inner)
        basis = jax.scipy.linalg.solve_triangular(factor, image.T, lower=True).T
    return basis


def local(signal, start_frames, start_sends, start_rows, start_cols, rank_frames, rank_sends):
    high = lax.Precision.HIGHEST
    rows_dev, cols_dev = (signal.shape[0], signal.shape[1])
    pixels = rows_dev * cols_dev
    flattened = signal.reshape(-1, NT)
    blocks = signal.reshape(pixels, NK, NT)
    local_frames = jnp.einsum("pt,pu->tu", flattened, flattened, precision=high)
    local_sends = jnp.einsum("pkt,pjt->kj", blocks, blocks, precision=high)
    small = jnp.pad(local_sends, ((0, 0), (0, 112))).reshape(2, 8, 128)
    tiles = all_sum(jnp.concatenate([packed(local_frames), small]), 1)
    gram_frames = unpacked(tiles[:48])
    gram_sends = tiles[48:].reshape(16, 128)[:, :16]
    keep_frames = (jnp.arange(TMAX, dtype=jnp.int32) < rank_frames[0]).astype(jnp.float32)
    keep_sends = (jnp.arange(KMAX, dtype=jnp.int32) < rank_sends[0]).astype(jnp.float32)
    basis_frames = orthonormal(gram_frames, start_frames) * keep_frames[None, :]
    basis_sends = orthonormal(gram_sends, start_sends) * keep_sends[None, :]
    reduced = jnp.dot(flattened, basis_frames, precision=high).reshape(pixels, NK, TMAX)
    core = jnp.einsum("pkb,ka->pab", reduced, basis_sends, precision=high)
    core = core.reshape(rows_dev, cols_dev, CORE_W)
    parts = core.reshape(rows_dev, cols_dev, NDEV, 2).transpose(2, 0, 1, 3)
    spread = lax.all_to_all(parts, ("row", "col"), 0, 0, tiled=True)
    spread = spread.reshape(16, 8, rows_dev, cols_dev, 2).transpose(0, 2, 1, 3, 4).reshape(256, 256, 2)
    unfolded = spread.reshape(256, -1)
    local_rows = jnp.dot(unfolded, unfolded.T, precision=high)
    gram_rows = unpacked(all_sum(packed(local_rows), 2))
    basis_rows = orthonormal(gram_rows, start_rows)
    second = jnp.dot(basis_rows.T, unfolded, precision=high).reshape(RS, 256, -1)
    local_cols = jnp.einsum("sce,sde->cd", second, second, precision=high)
    gram_cols = unpacked(all_sum(packed(local_cols), 3))
    basis_cols = orthonormal(gram_cols, start_cols)
    third = jnp.einsum("cu,sce->sue", basis_cols, second, precision=high)
    back_cols = jnp.einsum("cu,sue->sce", basis_cols, third, precision=high)
    projected = jnp.dot(basis_rows, back_cols.reshape(RS, -1), precision=high).reshape(spread.shape)
    parts = projected.reshape(16, rows_dev, 8, cols_dev, 2).transpose(0, 2, 1, 3, 4).reshape(NDEV, rows_dev, cols_dev, 2)
    back = lax.all_to_all(parts, ("row", "col"), 0, 0, tiled=True)
    tissue_core = back.transpose(1, 2, 0, 3).reshape(pixels, KMAX, TMAX)
    expanded = jnp.einsum("pab,ka->pkb", tissue_core, basis_sends, precision=high)
    tissue = jnp.dot(expanded.reshape(-1, TMAX), basis_frames.T, precision=high).reshape(
        signal.shape
    )
    return signal - tissue


def solution(mesh):
    return jax.shard_map(
        local,
        mesh=mesh,
        in_specs=(P("row", "col", None, None), P(), P(), P(), P(), P(), P()),
        out_specs=P("row", "col", None, None),
        check_vma=False,
    )
```

```python
import functools

import jax
import jax.numpy as jnp
from jax import lax
from jax.experimental import pallas as pl
from jax.experimental.pallas import tpu as pltpu
from jax.sharding import PartitionSpec as P

NT = 256
NK = 16
TMAX = 32
KMAX = 8
RS = 64
ITERS = 2
NDEV = 128
ROWS = 16
COLS = 32
LINES = COLS * NK
MESH = pl.DeviceIdType.MESH
F32 = jnp.float32
BF16 = jnp.bfloat16
HIGH = lax.Precision.HIGHEST


def me_index():
    return lax.axis_index("row") * 8 + lax.axis_index("col")


def coords(dev):
    return (dev // 8, dev % 8)


def dot(a, b, over=(1, 0)):
    dims = (((over[0],), (over[1],)), ((), ()))
    return lax.dot_general(a, b, dims, preferred_element_type=F32)


def full_dot(a, b, over=(1, 0)):
    dims = (((over[0],), (over[1],)), ((), ()))
    return lax.dot_general(a, b, dims, precision=HIGH, preferred_element_type=F32)


def halves(x):
    hi = x.astype(BF16)
    return hi, (x - hi.astype(F32)).astype(BF16)


def dot3(a, b, over=(1, 0)):
    a_hi, a_lo = halves(a)
    b_hi, b_lo = halves(b)
    return dot(a_hi, b_hi, over) + dot(a_hi, b_lo, over) + dot(a_lo, b_hi, over)


def self_dot(a):
    hi, lo = halves(a)
    side = dot(hi, lo, (1, 1))
    return dot(hi, hi, (1, 1)) + side + side.T


def remote(src, dst, send, recv, dev):
    return pltpu.make_async_remote_copy(
        src_ref=src, dst_ref=dst, send_sem=send, recv_sem=recv, device_id=coords(dev), device_id_type=MESH
    )


def wait_for(ref, count, sem):
    some = ref.at[pl.ds(0, count)]
    pltpu.make_async_copy(some, some, sem).wait()


def all_sum(me, pieces, part, inbox, total, sems):
    chip = me // 2
    reducer = jnp.logical_and(me % 2 == 1, chip < pieces)
    first = chip % pieces

    def scatter(s, _):
        piece = (first + s) % pieces
        dev = 2 * piece + 1

        @pl.when(dev != me)
        def _():
            slot = (me - dev + 2 * NDEV - 1) % NDEV
            remote(part.at[piece], inbox.at[slot], sems.at[0], sems.at[1], dev).start()

        return 0

    lax.fori_loop(0, pieces, scatter, 0)

    @pl.when(reducer)
    def _():
        wait_for(inbox, NDEV - 1, sems.at[1])
        lanes = [inbox[i] for i in range(4)]
        for i in range(4, NDEV - 1):
            lanes[i % 4] = lanes[i % 4] + inbox[i]
        total[chip] = (lanes[0] + lanes[1]) + (lanes[2] + lanes[3]) + part[chip]

        def spread(s, _):
            dev = (me + s) % NDEV
            remote(total.at[chip], total.at[chip], sems.at[2], sems.at[3], dev).start()
            return 0

        lax.fori_loop(1, NDEV, spread, 0)
        wait_for(part, pieces - 1, sems.at[3])
        wait_for(part, pieces - 1, sems.at[0])
        wait_for(inbox, NDEV - 1, sems.at[2])

    @pl.when(jnp.logical_not(reducer))
    def _():
        wait_for(part, pieces, sems.at[3])
        wait_for(part, pieces, sems.at[0])


def pack(gram, part):
    part[0:16] = gram[:128, :128].reshape(16, 8, 128)
    part[16:32] = gram[:128, 128:].reshape(16, 8, 128)
    part[32:48] = gram[128:, 128:].reshape(16, 8, 128)


def unpack(total, gram):
    corner = total[16:32].reshape(128, 128)
    gram[:128, :128] = total[0:16].reshape(128, 128)
    gram[:128, 128:] = corner
    gram[128:, :128] = corner.T
    gram[128:, 128:] = total[32:48].reshape(128, 128)


def inverse_factor(inner, size):
    groups = size // 8
    lane = lax.broadcasted_iota(jnp.int32, (8, 128), 1)
    sub = lax.broadcasted_iota(jnp.int32, (8, 128), 0)
    rest = [inner[8 * g : 8 * g + 8] for g in range(groups)]
    inv = [jnp.where(lane == sub + 8 * g, 1.0, 0.0).astype(F32) for g in range(groups)]

    def row(x, j):
        return jnp.broadcast_to(x[j : j + 1], (8, 128))

    for b in range(groups):
        cols = [
            [jnp.broadcast_to(rest[g][:, 8 * b + j : 8 * b + j + 1], (8, 128)) for g in range(b, groups)]
            for j in range(8)
        ]
        pivots = jnp.ones((8, 128), F32)
        for j in range(8):
            pivot = row(cols[j][0], j)
            pivots = jnp.where(sub == j, pivot, pivots)
            scale = 1.0 / pivot
            heads = [row(cols[q][0], j) for q in range(j + 1, 8)]
            rest_row = row(rest[b], j)
            inv_row = row(inv[b], j)
            for g in range(b, groups):
                step = cols[j][g - b] * scale
                if g == b:
                    step = jnp.where(sub > j, step, 0.0)
                else:
                    rest[g] = rest[g] - step * rest_row
                inv[g] = inv[g] - step * inv_row
                for q in range(j + 1, 8):
                    cols[q][g - b] = cols[q][g - b] - step * heads[q - j - 1]
                if g == b:
                    rest[g] = rest[g] - step * rest_row
        inv[b] = inv[b] * lax.rsqrt(pivots)
    return jnp.concatenate(inv, axis=0) if groups > 1 else inv[0]


def factor_step(image, size):
    inner = full_dot(image, image, (0, 0))
    return inverse_factor(inner[:size], size)


def orth(gram, basis, basis_t, size):
    def step(_, c):
        image = full_dot(gram[...], basis[...])
        lower = factor_step(image, size)
        basis[:, :size] = full_dot(image, lower, (1, 1))
        basis_t[...] = full_dot(lower, image, (1, 1))
        return c

    lax.fori_loop(0, ITERS, step, 0)


def swap(x):
    return pltpu.roll(x, 64, 1)


def regroup(a, b):
    left = lax.broadcasted_iota(jnp.int32, a.shape, 1) < 64
    return jnp.where(left, a, swap(b)), jnp.where(left, swap(a), b)


def main_kernel(
    x_hbm, start_f, start_s, start_r, start_c, rank_f, rank_s,
    mixed_out, frames_out,
    xin, xhi, xlo, acc, side, acc_s, side_s, gram, part_f, part_r, part_c,
    in_f, in_r, in_c, tot_f, tot_r, tot_c, bf, bft, bs, bst, br, brt, bc, bct,
    red, kron, send1, recv1, unf, send2, recv2,
    load_sems, sems, swap_sems,
):
    me = me_index()
    mine_row, mine_col = lax.axis_index("row"), lax.axis_index("col")
    for r in range(ROWS):
        pltpu.make_async_copy(x_hbm.at[r], xin.at[r], load_sems.at[r]).start()
    barrier = pltpu.get_barrier_semaphore()

    def greet(s, c):
        pl.semaphore_signal(barrier, inc=1, device_id=coords((me + s) % NDEV), device_id_type=MESH)
        return c

    lax.fori_loop(1, NDEV, greet, 0)

    acc[...] = jnp.zeros_like(acc)
    side[...] = jnp.zeros_like(side)
    acc_s[...] = jnp.zeros_like(acc_s)
    side_s[...] = jnp.zeros_like(side_s)
    for ref, start in ((bf, start_f), (br, start_r), (bc, start_c), (bs, start_s)):
        ref[...] = jnp.zeros_like(ref)
    bf[:, :TMAX] = start_f[...]
    bs[:NK, :KMAX] = start_s[...]
    rows_start = start_r[...].reshape(16, 2, 8, RS)
    br[:128, :RS] = rows_start[:, 0].reshape(128, RS)
    br[128:, :RS] = rows_start[:, 1].reshape(128, RS)
    bc[:, :RS] = start_c[...]

    def gather(r, c):
        pltpu.make_async_copy(x_hbm.at[r], xin.at[r], load_sems.at[r]).wait()
        hi, lo = halves(xin[r])
        xhi[r] = hi
        xlo[r] = lo
        acc[...] += dot(hi, hi, (0, 0))
        side[...] += dot(hi, lo, (0, 0))
        acc_s[...] += dot(hi[:256], hi[:256], (1, 1)) + dot(hi[256:], hi[256:], (1, 1))
        side_s[...] += dot(hi[:256], lo[:256], (1, 1)) + dot(hi[256:], lo[256:], (1, 1))
        return c

    lax.fori_loop(0, ROWS, gather, 0)
    pack(acc[...] + side[...] + side[...].T, part_f)
    sends = acc_s[...] + side_s[...] + side_s[...].T
    i0 = lax.broadcasted_iota(jnp.int32, (256, 256), 0)
    i1 = lax.broadcasted_iota(jnp.int32, (256, 256), 1)
    sends = jnp.where(i0 // NK == i1 // NK, sends, 0.0).reshape(16, NK, 256).sum(axis=0)
    j0 = lax.broadcasted_iota(jnp.int32, (256, 128), 0)
    j1 = lax.broadcasted_iota(jnp.int32, (256, 128), 1)
    part_f[48:50] = full_dot(sends, (j0 % NK == j1).astype(F32)).reshape(2, 8, 128)

    pl.semaphore_wait(barrier, NDEV - 1)
    all_sum(me, 50, part_f, in_f, tot_f, sems.at[0])

    unpack(tot_f, gram)

    def both(_, c):
        image = full_dot(gram[...], bf[...])
        small = full_dot(tot_f[48:50].reshape(NK, 128), bs[...])
        lower = factor_step(image, TMAX)
        lower_s = factor_step(small, KMAX)
        bf[:, :TMAX] = full_dot(image, lower, (1, 1))
        bft[...] = full_dot(lower, image, (1, 1))
        bs[:NK, :KMAX] = full_dot(small, lower_s, (1, 1))
        return c

    lax.fori_loop(0, ITERS, both, 0)
    keep_f = lax.broadcasted_iota(jnp.int32, (TMAX, NT), 0) < rank_f[0]
    frames_t = bft[...] * keep_f.astype(F32)
    frames_out[...] = frames_t
    keep_s = lax.broadcasted_iota(jnp.int32, (128, 128), 1) < rank_s[0]
    sends = bs[...] * keep_s.astype(F32)
    a0 = lax.broadcasted_iota(jnp.int32, (128, 256), 0)
    a1 = lax.broadcasted_iota(jnp.int32, (128, 256), 1)
    wide = full_dot(sends[:NK], (a0 == a1 // COLS).astype(F32))
    c0 = lax.broadcasted_iota(jnp.int32, (LINES, 256), 0)
    c1 = lax.broadcasted_iota(jnp.int32, (LINES, 256), 1)
    kron[...] = jnp.where(c0 // NK == c1 % COLS, jnp.concatenate([wide] * COLS, axis=0), 0.0)

    f_hi, f_lo = halves(frames_t)
    f_two = jnp.concatenate([f_hi, f_lo], axis=0)
    for r in range(ROWS):
        both_ways = dot(f_two, xhi[r], (1, 1))
        here = both_ways[:TMAX] + both_ways[TMAX:] + dot(f_hi, xlo[r], (1, 1))
        for q in range(4):
            red[q, pl.ds((r // 8) * 256 + r % 8, TMAX, stride=8), :] = here[:, 128 * q : 128 * q + 128]
    core = dot3(jnp.concatenate([red[q] for q in range(4)], axis=1), kron[...])
    for t in range(2):
        lanes = slice(128 * t, 128 * t + 128)
        one, two = regroup(core[:256, lanes], core[256:, lanes])
        send1[32 * t : 32 * t + 32] = one.reshape(32, 8, 128)
        send1[64 + 32 * t : 96 + 32 * t] = two.reshape(32, 8, 128)

    own = mine_col * 16 + mine_row
    recv1[own] = send1[me]

    def deal(s, c):
        dev = (me + s) % NDEV
        remote(send1.at[dev], recv1.at[own], swap_sems.at[0], swap_sems.at[1], dev).start()
        return c

    lax.fori_loop(1, NDEV, deal, 0)
    wait_for(recv1, NDEV - 1, swap_sems.at[1])

    for p in range(4):
        lanes = slice(128 * p, 128 * p + 128)
        one, two = regroup(
            recv1[32 * p : 32 * p + 16].reshape(128, 128), recv1[32 * p + 16 : 32 * p + 32].reshape(128, 128)
        )
        unf[:128, lanes] = one
        unf[128:, lanes] = two
    pack(self_dot(unf[...]), part_r)
    all_sum(me, 48, part_r, in_r, tot_r, sems.at[1])
    unpack(tot_r, gram)
    orth(gram, br, brt, RS)

    second = dot3(brt[...], unf[...])
    turned = second.T.reshape(8, 2, 32, RS)
    cols = [turned[:, e].reshape(256, RS) for e in range(2)]
    pack(self_dot(cols[0]) + self_dot(cols[1]), part_c)
    all_sum(me, 48, part_c, in_c, tot_c, sems.at[2])
    unpack(tot_c, gram)
    orth(gram, bc, bct, RS)

    backs = []
    for e in range(2):
        third = dot3(bct[...], cols[e])
        backs.append(dot3(bc[:, :RS], third).reshape(8, 1, 32, RS))
    back = jnp.concatenate(backs, axis=1).reshape(512, RS)
    projected = dot3(br[:, :RS], back, (1, 1))
    for p in range(4):
        lanes = slice(128 * p, 128 * p + 128)
        one, two = regroup(projected[:128, lanes], projected[128:, lanes])
        send2[32 * p : 32 * p + 16] = one.reshape(16, 8, 128)
        send2[32 * p + 16 : 32 * p + 32] = two.reshape(16, 8, 128)
    recv2[me] = send2[own]

    def hand_back(s, c):
        dev = (me + s) % NDEV
        place = (dev % 8) * 16 + dev // 8
        remote(send2.at[place], recv2.at[me], swap_sems.at[2], swap_sems.at[3], dev).start()
        return c

    lax.fori_loop(1, NDEV, hand_back, 0)
    wait_for(recv2, NDEV - 1, swap_sems.at[3])
    upper, lower = [], []
    for t in range(2):
        one, two = regroup(
            recv2[32 * t : 32 * t + 32].reshape(256, 128), recv2[64 + 32 * t : 96 + 32 * t].reshape(256, 128)
        )
        upper.append(one)
        lower.append(two)
    whole = jnp.concatenate([jnp.concatenate(upper, axis=1), jnp.concatenate(lower, axis=1)], axis=0)
    mixed_out[...] = dot3(whole, kron[...], (1, 1))
    wait_for(send1, NDEV - 1, swap_sems.at[0])
    wait_for(send2, NDEV - 1, swap_sems.at[2])


def last_kernel(x_ref, mixed, frames, out_ref):
    r = pl.program_id(0)
    m_hi, m_lo = halves(mixed[...])
    f_hi, f_lo = halves(frames[...])
    tall = jnp.concatenate([m_hi, m_lo, m_hi], axis=0)
    flat = jnp.concatenate([f_hi, f_hi, f_lo], axis=0)
    out_ref[0] = x_ref[0] - dot(tall, flat, (0, 0))


def local(signal, start_frames, start_sends, start_rows, start_cols, rank_frames, rank_sends):
    x = signal.reshape(ROWS, LINES, NT)
    vmem = pl.BlockSpec(memory_space=pltpu.VMEM)
    smem = pl.BlockSpec(memory_space=pltpu.SMEM)
    tiles = lambda n: pltpu.VMEM((n, 8, 128), F32)
    flat = lambda *dims: pltpu.VMEM(dims, F32)
    mixed, frames = pl.pallas_call(
        main_kernel,
        out_shape=(jax.ShapeDtypeStruct((512, 512), F32), jax.ShapeDtypeStruct((TMAX, NT), F32)),
        in_specs=[pl.BlockSpec(memory_space=pl.ANY), vmem, vmem, vmem, vmem, smem, smem],
        out_specs=(vmem, vmem),
        scratch_shapes=[
            flat(ROWS, LINES, NT), pltpu.VMEM((ROWS, LINES, NT), BF16), pltpu.VMEM((ROWS, LINES, NT), BF16),
            flat(256, 256), flat(256, 256), flat(256, 256), flat(256, 256), flat(256, 256),
            tiles(50), tiles(48), tiles(48), tiles(NDEV - 1), tiles(NDEV - 1), tiles(NDEV - 1),
            tiles(50), tiles(48), tiles(48),
            flat(256, 128), flat(TMAX, 256), flat(128, 128), flat(8, 128),
            flat(256, 128), flat(RS, 256), flat(256, 128), flat(RS, 256),
            flat(4, 512, 128), flat(512, 256), tiles(NDEV), tiles(NDEV), flat(256, 512), tiles(NDEV), tiles(NDEV),
            pltpu.SemaphoreType.DMA((ROWS,)), pltpu.SemaphoreType.DMA((3, 4)), pltpu.SemaphoreType.DMA((4,)),
        ],
        compiler_params=pltpu.CompilerParams(
            collective_id=1, has_side_effects=True, vmem_limit_bytes=56 * 1024 * 1024
        ),
        name="modes",
    )(x, start_frames, start_sends, start_rows, start_cols, rank_frames, rank_sends)
    mixed = mixed.reshape(2, TMAX, 8, LINES).transpose(0, 2, 1, 3).reshape(512, 512)
    out = pl.pallas_call(
        last_kernel,
        grid=(ROWS,),
        out_shape=jax.ShapeDtypeStruct(x.shape, F32),
        in_specs=[
            pl.BlockSpec((1, LINES, NT), lambda r: (r, 0, 0)),
            pl.BlockSpec((TMAX, LINES), lambda r: (r, 0)),
            pl.BlockSpec((TMAX, NT), lambda r: (0, 0)),
        ],
        out_specs=pl.BlockSpec((1, LINES, NT), lambda r: (r, 0, 0)),
        compiler_params=pltpu.CompilerParams(dimension_semantics=("arbitrary",)),
        name="subtract",
    )(x, mixed, frames)
    return out.reshape(signal.shape)


def solution(mesh):
    return jax.shard_map(
        local,
        mesh=mesh,
        in_specs=(P("row", "col", None, None), P(), P(), P(), P(), P(), P()),
        out_specs=P("row", "col", None, None),
        check_vma=False,
    )
```

```python
import functools

import jax
import jax.numpy as jnp
from jax import lax
from jax.experimental import pallas as pl
from jax.experimental.pallas import tpu as pltpu
from jax.sharding import PartitionSpec as P

NT = 256
NK = 16
TMAX = 32
KMAX = 8
RS = 64
ITERS = 2
NDEV = 128
ROWS = 16
COLS = 32
LINES = COLS * NK
MESH = pl.DeviceIdType.MESH
F32 = jnp.float32
BF16 = jnp.bfloat16
HIGH = lax.Precision.HIGHEST


def me_index():
    return lax.axis_index("row") * 8 + lax.axis_index("col")


def dot(a, b, over=(1, 0)):
    dims = (((over[0],), (over[1],)), ((), ()))
    return lax.dot_general(a, b, dims, preferred_element_type=F32)


def full_dot(a, b, over=(1, 0)):
    dims = (((over[0],), (over[1],)), ((), ()))
    return lax.dot_general(a, b, dims, precision=HIGH, preferred_element_type=F32)


def halves(x):
    hi = x.astype(BF16)
    return hi, (x - hi.astype(F32)).astype(BF16)


def dot3(a, b, over=(1, 0)):
    a_hi, a_lo = halves(a)
    b_hi, b_lo = halves(b)
    return dot(a_hi, b_hi, over) + dot(a_hi, b_lo, over) + dot(a_lo, b_hi, over)


def self_dot(a):
    hi, lo = halves(a)
    side = dot(hi, lo, (1, 1))
    return dot(hi, hi, (1, 1)) + side + side.T


def remote(src, dst, send, recv, dev):
    return pltpu.make_async_remote_copy(
        src_ref=src, dst_ref=dst, send_sem=send, recv_sem=recv, device_id=dev, device_id_type=MESH
    )


def wait_for(ref, count, sem):
    some = ref.at[pl.ds(0, count)]
    pltpu.make_async_copy(some, some, sem).wait()


HOPS = (0, 1, 2, 1)
CHIPS = sorted(
    [(x, y, z) for x in range(4) for y in range(4) for z in range(4)], key=lambda o: -sum(HOPS[i] for i in o)
)
PEERS = [(x, y, z, k) for x, y, z in CHIPS for k in range(2) if x + y + z + k]


def places():
    row, col = lax.axis_index("row"), lax.axis_index("col")
    x, y, z, k = lax.div(row, 4), lax.rem(row, 4), lax.div(col, 2), lax.rem(col, 2)
    rows = [[lax.rem(x + dx, 4) * 4 + lax.rem(y + dy, 4) for dy in range(4)] for dx in range(4)]
    planes = [lax.rem(z + dz, 4) for dz in range(4)]
    cols = [[planes[dz] * 2 + lax.rem(k + dk, 2) for dk in range(2)] for dz in range(4)]
    return rows, cols, planes, k


def all_sum(where, part, inbox, total, sems):
    rows, cols, planes, k = where
    for place, (dx, dy, dz) in enumerate(CHIPS):
        row, plane = rows[dx][dy], planes[dz]
        copy = remote(
            part.at[row * 4 + plane], inbox.at[2 * place + k], sems.at[0], sems.at[1], (row, plane * 2 + 1)
        )
        if dx + dy + dz:
            copy.start()
        else:
            pl.when(k == 0)(copy.start)

    @pl.when(k == 1)
    def _():
        piece = rows[0][0] * 4 + planes[0]
        wait_for(inbox, NDEV - 1, sems.at[1])
        lanes = [inbox[i] for i in range(4)]
        for i in range(4, NDEV - 1):
            lanes[i % 4] = lanes[i % 4] + inbox[i]
        total[piece] = (lanes[0] + lanes[1]) + (lanes[2] + lanes[3]) + part[piece]
        for dx, dy, dz, dk in PEERS:
            remote(total.at[piece], total.at[piece], sems.at[2], sems.at[3], (rows[dx][dy], cols[dz][dk])).start()
        wait_for(part, 63, sems.at[3])

    @pl.when(k == 0)
    def _():
        wait_for(part, 64, sems.at[3])

    def finish():
        @pl.when(k == 1)
        def _():
            wait_for(part, 63, sems.at[0])
            wait_for(inbox, NDEV - 1, sems.at[2])

        @pl.when(k == 0)
        def _():
            wait_for(part, 64, sems.at[0])

    return finish


def pack(gram, part, extra=None):
    corner = gram[128:, 128:]
    if extra is not None:
        lane = lax.broadcasted_iota(jnp.int32, (NK, 128), 1)
        corner = jnp.concatenate([corner[: 128 - NK], jnp.where(lane < NK, extra, corner[128 - NK :])], axis=0)
    lines = jnp.concatenate([gram[:128, :128], gram[:128, 128:], corner], axis=0)
    for p in range(64):
        part[p] = lines[6 * p : 6 * p + 6]


def unpack(total, stage, gram, extra=None):
    for p in range(64):
        stage[6 * p : 6 * p + 6] = total[p]
    side = stage[128:256]
    gram[:128, :128] = stage[:128]
    gram[:128, 128:] = side
    gram[128:, :128] = side.T
    gram[128:, 128:] = stage[256:]
    if extra is not None:
        extra[...] = stage[384 - NK :, :NK]
        lane = lax.broadcasted_iota(jnp.int32, (NK, 128), 1)
        turned = stage[256:].T[128 - NK :]
        gram[256 - NK :, 128:] = jnp.where(lane < NK, turned, stage[384 - NK :])


def inverse_factor(inner, size):
    groups = size // 8
    lane = lax.broadcasted_iota(jnp.int32, (8, size), 1)
    sub = lax.broadcasted_iota(jnp.int32, (8, size), 0)
    rest = [inner[8 * g : 8 * g + 8] for g in range(groups)]
    inv = [jnp.where(lane == sub + 8 * g, 1.0, 0.0).astype(F32) for g in range(groups)]

    def row(x, j):
        return jnp.broadcast_to(x[j : j + 1], (8, size))

    for b in range(groups):
        cols = [
            [jnp.broadcast_to(rest[g][:, 8 * b + j : 8 * b + j + 1], (8, size)) for g in range(b, groups)]
            for j in range(8)
        ]
        pivots = jnp.ones((8, size), F32)
        for j in range(8):
            pivot = row(cols[j][0], j)
            pivots = jnp.where(sub == j, pivot, pivots)
            scale = 1.0 / pivot
            heads = [row(cols[q][0], j) for q in range(j + 1, 8)]
            rest_row = row(rest[b], j)
            inv_row = row(inv[b], j)
            for g in range(b, groups):
                step = cols[j][g - b] * scale
                if g == b:
                    step = jnp.where(sub > j, step, 0.0)
                for q in range(j + 1, 8):
                    cols[q][g - b] = cols[q][g - b] - step * heads[q - j - 1]
                rest[g] = rest[g] - step * rest_row
                inv[g] = inv[g] - step * inv_row
        inv[b] = inv[b] * lax.rsqrt(pivots)
    return jnp.concatenate(inv, axis=0) if groups > 1 else inv[0]


def next_basis(image):
    lower = inverse_factor(full_dot(image, image, (1, 1)), image.shape[0])
    return full_dot(lower, image)


def orth(gram, basis):
    def step(_, c):
        basis[...] = next_basis(full_dot(basis[...], gram[...]))
        return c

    lax.fori_loop(0, ITERS, step, 0)


def swap(x):
    return pltpu.roll(x, 64, 1)


def regroup(a, b):
    left = lax.broadcasted_iota(jnp.int32, a.shape, 1) < 64
    return jnp.where(left, a, swap(b)), jnp.where(left, swap(a), b)


def main_kernel(
    x_hbm, start_f, start_s, start_r, start_c, rank_f, rank_s,
    xin, mixed_out, frames_out,
    xhi, xlo, acc, side, acc_s, side_s, gram, part_f, part_r, part_c,
    in_f, in_r, in_c, tot_f, tot_r, tot_c, stage, gram_s, bft, bst, brt, bct,
    red, kron, back, send1, recv1, unf, send2, recv2,
    load_sems, start_sems, sems, swap_sems,
):
    me = me_index()
    mine_row, mine_col = lax.axis_index("row"), lax.axis_index("col")
    for r in range(ROWS):
        pltpu.make_async_copy(x_hbm.at[r], xin.at[r], load_sems.at[r]).start()
    starts = [
        pltpu.make_async_copy(start, ref, start_sems.at[i])
        for i, (ref, start) in enumerate(((bft, start_f), (bst, start_s), (brt, start_r), (bct, start_c)))
    ]
    for copy in starts:
        copy.start()
    barrier = pltpu.get_barrier_semaphore()

    where = places()
    rows_of, cols_of = where[0], where[1]
    for dx, dy, dz, dk in PEERS:
        pl.semaphore_signal(barrier, inc=1, device_id=(rows_of[dx][dy], cols_of[dz][dk]), device_id_type=MESH)

    acc[...] = jnp.zeros_like(acc)
    side[...] = jnp.zeros_like(side)
    acc_s[...] = jnp.zeros_like(acc_s)
    side_s[...] = jnp.zeros_like(side_s)
    def gather(r, c):
        pltpu.make_async_copy(x_hbm.at[r], xin.at[r], load_sems.at[r]).wait()
        hi, lo = halves(xin[r])
        xhi[r] = hi
        xlo[r] = lo
        acc[...] += dot(hi, hi, (0, 0))
        side[...] += dot(hi, lo, (0, 0))
        acc_s[...] += dot(hi[:256], hi[:256], (1, 1)) + dot(hi[256:], hi[256:], (1, 1))
        side_s[...] += dot(hi[:256], lo[:256], (1, 1)) + dot(hi[256:], lo[256:], (1, 1))
        return c

    lax.fori_loop(0, ROWS, gather, 0)
    sends = acc_s[...] + side_s[...] + side_s[...].T
    i0 = lax.broadcasted_iota(jnp.int32, (256, 256), 0)
    i1 = lax.broadcasted_iota(jnp.int32, (256, 256), 1)
    sends = jnp.where(i0 // NK == i1 // NK, sends, 0.0).reshape(16, NK, 256).sum(axis=0)
    j0 = lax.broadcasted_iota(jnp.int32, (256, 128), 0)
    j1 = lax.broadcasted_iota(jnp.int32, (256, 128), 1)
    small = full_dot(sends, (j0 % NK == j1).astype(F32))
    pack(acc[...] + side[...] + side[...].T, part_f, small)

    for copy in starts:
        copy.wait()
    pl.semaphore_wait(barrier, NDEV - 1)
    finish_f = all_sum(where, part_f, in_f, tot_f, sems.at[0])

    unpack(tot_f, stage, gram, gram_s)

    def both(_, c):
        image = full_dot(bft[...], gram[...])
        small = full_dot(bst[...], gram_s[...])
        bft[...] = next_basis(image)
        bst[...] = next_basis(small)
        return c

    lax.fori_loop(0, ITERS, both, 0)
    keep_f = lax.broadcasted_iota(jnp.int32, (TMAX, NT), 0) < rank_f[0]
    frames_t = bft[...] * keep_f.astype(F32)
    frames_out[...] = frames_t
    keep_s = lax.broadcasted_iota(jnp.int32, (KMAX, NK), 0) < rank_s[0]
    sends = bst[...] * keep_s.astype(F32)
    a0 = lax.broadcasted_iota(jnp.int32, (KMAX, 256), 0)
    a1 = lax.broadcasted_iota(jnp.int32, (KMAX, 256), 1)
    wide = full_dot(sends, (a0 == a1 // COLS).astype(F32), (0, 0))
    c0 = lax.broadcasted_iota(jnp.int32, (LINES, 256), 0)
    c1 = lax.broadcasted_iota(jnp.int32, (LINES, 256), 1)
    spread = jnp.where(c0 // NK == c1 % COLS, jnp.concatenate([wide] * COLS, axis=0), 0.0)
    kron[0] = spread[:, :128]
    kron[1] = spread[:, 128:]

    f_hi, f_lo = halves(frames_t)
    f_two = jnp.concatenate([f_hi, f_lo], axis=0)
    for r in range(ROWS):
        both_ways = dot(f_two, xhi[r], (1, 1))
        here = both_ways[:TMAX] + both_ways[TMAX:] + dot(f_hi, xlo[r], (1, 1))
        for q in range(4):
            red[q, pl.ds((r // 8) * 256 + r % 8, TMAX, stride=8), :] = here[:, 128 * q : 128 * q + 128]
    own = mine_col * 16 + mine_row
    parity = lax.rem(lax.div(mine_row, 4), 2)
    r_hi, r_lo = halves(jnp.concatenate([red[q] for q in range(4)], axis=1))
    for odd in range(2):
        t = 1 - parity if odd else parity
        k_hi, k_lo = halves(kron[t])
        core = dot(r_hi, k_hi) + dot(r_hi, k_lo) + dot(r_lo, k_hi)
        one, two = regroup(core[:256], core[256:])
        send1[pl.ds(32 * t, 32)] = one.reshape(32, 8, 128)
        send1[pl.ds(64 + 32 * t, 32)] = two.reshape(32, 8, 128)
        if not odd:
            recv1[own] = send1[me]
        for dx, dy, dz, dk in PEERS:
            if dx % 2 == odd:
                row, col = rows_of[dx][dy], cols_of[dz][dk]
                remote(send1.at[row * 8 + col], recv1.at[own], swap_sems.at[0], swap_sems.at[1], (row, col)).start()
    wait_for(recv1, NDEV - 1, swap_sems.at[1])

    for p in range(4):
        lanes = slice(128 * p, 128 * p + 128)
        one, two = regroup(
            recv1[32 * p : 32 * p + 16].reshape(128, 128), recv1[32 * p + 16 : 32 * p + 32].reshape(128, 128)
        )
        both_halves = [one.reshape(16, 1, 8, 128), two.reshape(16, 1, 8, 128)]
        unf[:, lanes] = jnp.concatenate(both_halves, axis=1).reshape(256, 128)
    pack(self_dot(unf[...]), part_r)
    finish_r = all_sum(where, part_r, in_r, tot_r, sems.at[1])
    unpack(tot_r, stage, gram)
    orth(gram, brt)

    second = dot3(brt[...], unf[...])
    turned = second.T.reshape(8, 2, 32, RS)
    cols = [turned[:, e].reshape(256, RS) for e in range(2)]
    pack(self_dot(cols[0]) + self_dot(cols[1]), part_c)
    finish_c = all_sum(where, part_c, in_c, tot_c, sems.at[2])
    unpack(tot_c, stage, gram)
    orth(gram, bct)

    by_col, by_row = bct[...].T, brt[...].T
    backs = []
    for e in range(2):
        third = dot3(bct[...], cols[e])
        backs.append(dot3(by_col, third).reshape(8, 1, 32, RS))
    back[...] = jnp.concatenate(backs, axis=1).reshape(4, 128, RS)
    for near in (2, 1, 3, 0):
        p = where[2][near]
        pairs = dot3(by_row, back[p], (1, 1)).reshape(16, 2, 8, 128)
        one, two = regroup(pairs[:, 0].reshape(128, 128), pairs[:, 1].reshape(128, 128))
        send2[pl.ds(32 * p, 16)] = one.reshape(16, 8, 128)
        send2[pl.ds(32 * p + 16, 16)] = two.reshape(16, 8, 128)
        if near == 0:
            recv2[me] = send2[own]
        for dx, dy, dz, dk in PEERS:
            if dz == near:
                row, col = rows_of[dx][dy], cols_of[dz][dk]
                remote(send2.at[col * 16 + row], recv2.at[me], swap_sems.at[2], swap_sems.at[3], (row, col)).start()
    wait_for(recv2, NDEV - 1, swap_sems.at[3])
    upper, lower = [], []
    for t in range(2):
        one, two = regroup(
            recv2[32 * t : 32 * t + 32].reshape(256, 128), recv2[64 + 32 * t : 96 + 32 * t].reshape(256, 128)
        )
        upper.append(one)
        lower.append(two)
    whole = jnp.concatenate([jnp.concatenate(upper, axis=1), jnp.concatenate(lower, axis=1)], axis=0)
    mixed = dot3(whole, jnp.concatenate([kron[0], kron[1]], axis=1), (1, 1))
    for q in range(4):
        mixed_out[q] = mixed[:, 128 * q : 128 * q + 128]
    for finish in (finish_f, finish_r, finish_c):
        finish()
    wait_for(send1, NDEV - 1, swap_sems.at[0])
    wait_for(send2, NDEV - 1, swap_sems.at[2])


def last_kernel(x_ref, mixed, frames, out_hbm, o_buf, store_sems):
    f_hi, f_lo = halves(frames[...])
    flat = jnp.concatenate([f_hi, f_hi, f_lo], axis=0)
    for r in range(ROWS):
        lines = pl.ds((r // 8) * 256 + r % 8, TMAX, stride=8)
        m_hi, m_lo = halves(jnp.concatenate([mixed[q, lines, :] for q in range(4)], axis=1))
        tall = jnp.concatenate([m_hi, m_lo, m_hi], axis=0)
        o_buf[r] = x_ref[r] - dot(tall, flat, (0, 0))
        pltpu.make_async_copy(o_buf.at[r], out_hbm.at[r], store_sems.at[r]).start()
    for r in range(ROWS):
        pltpu.make_async_copy(o_buf.at[r], out_hbm.at[r], store_sems.at[r]).wait()


def local(signal, start_frames, start_sends, start_rows, start_cols, rank_frames, rank_sends):
    x = signal.reshape(ROWS, LINES, NT)
    vmem = pl.BlockSpec(memory_space=pltpu.VMEM)
    smem = pl.BlockSpec(memory_space=pltpu.SMEM)
    hbm = pl.BlockSpec(memory_space=pltpu.HBM)
    tiles = lambda n: pltpu.VMEM((n, 8, 128), F32)
    flat = lambda *dims: pltpu.VMEM(dims, F32)
    held, mixed, frames = pl.pallas_call(
        main_kernel,
        out_shape=(pltpu.VMEM(x.shape, F32), pltpu.VMEM((4, 512, 128), F32), pltpu.VMEM((TMAX, NT), F32)),
        in_specs=[hbm, hbm, hbm, hbm, hbm, smem, smem],
        out_specs=(vmem, vmem, vmem),
        scratch_shapes=[
            pltpu.VMEM((ROWS, LINES, NT), BF16), pltpu.VMEM((ROWS, LINES, NT), BF16),
            flat(256, 256), flat(256, 256), flat(256, 256), flat(256, 256), flat(256, 256),
            flat(64, 6, 128), flat(64, 6, 128), flat(64, 6, 128),
            flat(NDEV - 1, 6, 128), flat(NDEV - 1, 6, 128), flat(NDEV - 1, 6, 128),
            flat(64, 6, 128), flat(64, 6, 128), flat(64, 6, 128), flat(384, 128), flat(NK, NK),
            flat(TMAX, NT), flat(KMAX, NK), flat(RS, 256), flat(RS, 256),
            flat(4, 512, 128), flat(2, 512, 128), flat(4, 128, RS), tiles(NDEV), tiles(NDEV), flat(256, 512), tiles(NDEV), tiles(NDEV),
            pltpu.SemaphoreType.DMA((ROWS,)), pltpu.SemaphoreType.DMA((4,)), pltpu.SemaphoreType.DMA((3, 4)), pltpu.SemaphoreType.DMA((4,)),
        ],
        compiler_params=pltpu.CompilerParams(
            collective_id=1, has_side_effects=True, vmem_limit_bytes=57573376
        ),
        name="modes",
    )(x, start_frames.T, start_sends.T, start_rows.T, start_cols.T, rank_frames, rank_sends)
    out = pl.pallas_call(
        last_kernel,
        out_shape=jax.ShapeDtypeStruct(x.shape, F32),
        in_specs=[vmem, vmem, vmem],
        out_specs=pl.BlockSpec(memory_space=pl.ANY),
        scratch_shapes=[flat(ROWS, LINES, NT), pltpu.SemaphoreType.DMA((ROWS,))],
        compiler_params=pltpu.CompilerParams(vmem_limit_bytes=24 * 1024 * 1024),
        name="subtract",
    )(held, mixed, frames)
    return out.reshape(signal.shape)


def solution(mesh):
    return jax.shard_map(
        local,
        mesh=mesh,
        in_specs=(P("row", "col", None, None), P(), P(), P(), P(), P(), P()),
        out_specs=P("row", "col", None, None),
        check_vma=False,
    )
```

```python
import functools

import jax
import jax.numpy as jnp
from jax import lax
from jax.experimental import pallas as pl
from jax.experimental.pallas import tpu as pltpu
from jax.sharding import PartitionSpec as P

NT = 256
NK = 16
TMAX = 32
KMAX = 8
RS = 64
ITERS = 2
NDEV = 128
ROWS = 16
COLS = 32
LINES = COLS * NK
MESH = pl.DeviceIdType.MESH
F32 = jnp.float32
BF16 = jnp.bfloat16
HIGH = lax.Precision.HIGHEST


def me_index():
    return lax.axis_index("row") * 8 + lax.axis_index("col")


def dot(a, b, over=(1, 0)):
    dims = (((over[0],), (over[1],)), ((), ()))
    return lax.dot_general(a, b, dims, preferred_element_type=F32)


def full_dot(a, b, over=(1, 0)):
    dims = (((over[0],), (over[1],)), ((), ()))
    return lax.dot_general(a, b, dims, precision=HIGH, preferred_element_type=F32)


def halves(x):
    hi = x.astype(BF16)
    return hi, (x - hi.astype(F32)).astype(BF16)


def dot3(a, b, over=(1, 0)):
    return split_dot(halves(a), halves(b), over)


def split_dot(a, b, over=(1, 0)):
    (a_hi, a_lo), (b_hi, b_lo) = a, b
    return dot(a_hi, b_hi, over) + dot(a_hi, b_lo, over) + dot(a_lo, b_hi, over)


def self_dot(parts):
    hi, lo = parts
    side = dot(hi, lo, (1, 1))
    return dot(hi, hi, (1, 1)) + side + side.T


def remote(src, dst, send, recv, dev):
    return pltpu.make_async_remote_copy(
        src_ref=src, dst_ref=dst, send_sem=send, recv_sem=recv, device_id=dev, device_id_type=MESH
    )


def wait_for(ref, count, sem):
    some = ref.at[pl.ds(0, count)]
    pltpu.make_async_copy(some, some, sem).wait()


HOPS = (0, 1, 2, 1)
CHIPS = sorted(
    [(x, y, z) for x in range(4) for y in range(4) for z in range(4)], key=lambda o: -sum(HOPS[i] for i in o)
)
PEERS = [(x, y, z, k) for x, y, z in CHIPS for k in range(2) if x + y + z + k]


def places():
    row, col = lax.axis_index("row"), lax.axis_index("col")
    x, y, z, k = lax.div(row, 4), lax.rem(row, 4), lax.div(col, 2), lax.rem(col, 2)
    rows = [[lax.rem(x + dx, 4) * 4 + lax.rem(y + dy, 4) for dy in range(4)] for dx in range(4)]
    planes = [lax.rem(z + dz, 4) for dz in range(4)]
    cols = [[planes[dz] * 2 + lax.rem(k + dk, 2) for dk in range(2)] for dz in range(4)]
    return rows, cols, planes, k


def all_sum(where, part, inbox, total, sems):
    rows, cols, planes, k = where
    for place, (dx, dy, dz) in enumerate(CHIPS):
        row, plane = rows[dx][dy], planes[dz]
        copy = remote(
            part.at[row * 4 + plane], inbox.at[2 * place + k], sems.at[0], sems.at[1], (row, plane * 2 + 1)
        )
        if dx + dy + dz:
            copy.start()
        else:
            pl.when(k == 0)(copy.start)

    @pl.when(k == 1)
    def _():
        piece = rows[0][0] * 4 + planes[0]
        wait_for(inbox, NDEV - 1, sems.at[1])
        lanes = [inbox[i] for i in range(4)]
        for i in range(4, NDEV - 1):
            lanes[i % 4] = lanes[i % 4] + inbox[i]
        total[piece] = (lanes[0] + lanes[1]) + (lanes[2] + lanes[3]) + part[piece]
        for dx, dy, dz, dk in PEERS:
            remote(total.at[piece], total.at[piece], sems.at[2], sems.at[3], (rows[dx][dy], cols[dz][dk])).start()
        wait_for(part, 63, sems.at[3])

    @pl.when(k == 0)
    def _():
        wait_for(part, 64, sems.at[3])

    def finish():
        @pl.when(k == 1)
        def _():
            wait_for(part, 63, sems.at[0])
            wait_for(inbox, NDEV - 1, sems.at[2])

        @pl.when(k == 0)
        def _():
            wait_for(part, 64, sems.at[0])

    return finish


def pack(gram, part, extra=None):
    corner = gram[128:, 128:]
    if extra is not None:
        lane = lax.broadcasted_iota(jnp.int32, (NK, 128), 1)
        corner = jnp.concatenate([corner[: 128 - NK], jnp.where(lane < NK, extra, corner[128 - NK :])], axis=0)
    lines = jnp.concatenate([gram[:128, :128], gram[:128, 128:], corner], axis=0)
    for p in range(64):
        part[p] = lines[6 * p : 6 * p + 6]


def unpack(total, stage, gram, extra=None):
    for p in range(64):
        stage[6 * p : 6 * p + 6] = total[p]
    side = stage[128:256]
    gram[:128, :128] = stage[:128]
    gram[:128, 128:] = side
    gram[128:, :128] = side.T
    gram[128:, 128:] = stage[256:]
    if extra is not None:
        extra[...] = stage[384 - NK :, :NK]
        lane = lax.broadcasted_iota(jnp.int32, (NK, 128), 1)
        turned = stage[256:].T[128 - NK :]
        gram[256 - NK :, 128:] = jnp.where(lane < NK, turned, stage[384 - NK :])


def inverse_factor(inner, size):
    groups = size // 8
    lane = lax.broadcasted_iota(jnp.int32, (8, size), 1)
    sub = lax.broadcasted_iota(jnp.int32, (8, size), 0)
    rest = [inner[8 * g : 8 * g + 8] for g in range(groups)]
    inv = [jnp.where(lane == sub + 8 * g, 1.0, 0.0).astype(F32) for g in range(groups)]

    def row(x, j):
        return jnp.broadcast_to(x[j : j + 1], (8, size))

    def column(x, j):
        return jnp.broadcast_to(x[:, j : j + 1], (8, size))

    diag = [column(rest[0], q) for q in range(8)]
    for b in range(groups):
        below = range(b + 1, groups)
        cols = {(j, g): column(rest[g], 8 * b + j) for g in below for j in range(8)}
        ahead = [column(rest[b + 1], 8 * b + 8 + q) for q in range(8)] if below else None
        roots = jnp.ones((8, size), F32)
        for j in range(8):
            root = lax.rsqrt(row(diag[j], j))
            scale = root * root
            roots = jnp.where(sub == j, root, roots)
            heads = {q: row(diag[q], j) for q in range(j + 1, 8)}
            rest_row, inv_row = row(rest[b], j), row(inv[b], j)
            step = jnp.where(sub > j, diag[j] * scale, 0.0)
            for q in heads:
                diag[q] = diag[q] - step * heads[q]
            rest[b] = rest[b] - step * rest_row
            inv[b] = inv[b] - step * inv_row
            for g in below:
                side = cols[j, g]
                step = side * scale
                for q in heads:
                    cols[q, g] = cols[q, g] - step * heads[q]
                rest[g] = rest[g] - step * rest_row
                inv[g] = inv[g] - step * inv_row
                if g == b + 1:
                    for q in range(8):
                        ahead[q] = ahead[q] - step * row(side, q)
        inv[b] = inv[b] * roots
        diag = ahead
    return jnp.concatenate(inv, axis=0) if groups > 1 else inv[0]


def next_basis(image):
    lower = inverse_factor(full_dot(image, image, (1, 1)), image.shape[0])
    return full_dot(lower, image)


def orth(gram, basis):
    def step(_, c):
        basis[...] = next_basis(full_dot(basis[...], gram[...]))
        return c

    lax.fori_loop(0, ITERS, step, 0)


def swap(x):
    return pltpu.roll(x, 64, 1)


def regroup(a, b):
    left = lax.broadcasted_iota(jnp.int32, a.shape, 1) < 64
    return jnp.where(left, a, swap(b)), jnp.where(left, swap(a), b)


def main_kernel(
    x_hbm, start_f, start_s, start_r, start_c, rank_f, rank_s,
    xin, mixed_out, frames_out,
    xhi, xlo, acc, side, acc_s, side_s, gram, part_f, part_r, part_c,
    in_f, in_r, in_c, tot_f, tot_r, tot_c, stage, gram_s, bft, bst, brt, bct,
    red, kron_hi, kron_lo, back, send1, recv1, unf_hi, unf_lo, send2, recv2,
    load_sems, start_sems, sems, swap_sems,
):
    me = me_index()
    mine_row, mine_col = lax.axis_index("row"), lax.axis_index("col")
    for r in range(ROWS):
        pltpu.make_async_copy(x_hbm.at[r], xin.at[r], load_sems.at[r]).start()
    starts = [
        pltpu.make_async_copy(start, ref, start_sems.at[i])
        for i, (ref, start) in enumerate(((bft, start_f), (bst, start_s), (brt, start_r), (bct, start_c)))
    ]
    for copy in starts:
        copy.start()
    barrier = pltpu.get_barrier_semaphore()

    where = places()
    rows_of, cols_of = where[0], where[1]
    for dx, dy, dz, dk in PEERS:
        pl.semaphore_signal(barrier, inc=1, device_id=(rows_of[dx][dy], cols_of[dz][dk]), device_id_type=MESH)

    acc[...] = jnp.zeros_like(acc)
    side[...] = jnp.zeros_like(side)
    acc_s[...] = jnp.zeros_like(acc_s)
    side_s[...] = jnp.zeros_like(side_s)
    def gather(r, c):
        pltpu.make_async_copy(x_hbm.at[r], xin.at[r], load_sems.at[r]).wait()
        hi, lo = halves(xin[r])
        xhi[r] = hi
        xlo[r] = lo
        acc[...] += dot(hi, hi, (0, 0))
        side[...] += dot(hi, lo, (0, 0))
        acc_s[...] += dot(hi[:256], hi[:256], (1, 1)) + dot(hi[256:], hi[256:], (1, 1))
        side_s[...] += dot(hi[:256], lo[:256], (1, 1)) + dot(hi[256:], lo[256:], (1, 1))
        return c

    lax.fori_loop(0, ROWS, gather, 0)
    sends = acc_s[...] + side_s[...] + side_s[...].T
    i0 = lax.broadcasted_iota(jnp.int32, (256, 256), 0)
    i1 = lax.broadcasted_iota(jnp.int32, (256, 256), 1)
    sends = jnp.where(i0 // NK == i1 // NK, sends, 0.0).reshape(16, NK, 256).sum(axis=0)
    j0 = lax.broadcasted_iota(jnp.int32, (256, 128), 0)
    j1 = lax.broadcasted_iota(jnp.int32, (256, 128), 1)
    small = full_dot(sends, (j0 % NK == j1).astype(F32))
    pack(acc[...] + side[...] + side[...].T, part_f, small)

    for copy in starts:
        copy.wait()
    pl.semaphore_wait(barrier, NDEV - 1)
    finish_f = all_sum(where, part_f, in_f, tot_f, sems.at[0])

    unpack(tot_f, stage, gram, gram_s)

    def both(_, c):
        image = full_dot(bft[...], gram[...])
        small = full_dot(bst[...], gram_s[...])
        bft[...] = next_basis(image)
        bst[...] = next_basis(small)
        return c

    lax.fori_loop(0, ITERS, both, 0)
    keep_f = lax.broadcasted_iota(jnp.int32, (TMAX, NT), 0) < rank_f[0]
    frames_t = bft[...] * keep_f.astype(F32)
    frames_out[...] = frames_t
    keep_s = lax.broadcasted_iota(jnp.int32, (KMAX, NK), 0) < rank_s[0]
    sends = bst[...] * keep_s.astype(F32)
    a0 = lax.broadcasted_iota(jnp.int32, (KMAX, 256), 0)
    a1 = lax.broadcasted_iota(jnp.int32, (KMAX, 256), 1)
    wide = full_dot(sends, (a0 == a1 // COLS).astype(F32), (0, 0))
    c0 = lax.broadcasted_iota(jnp.int32, (LINES, 256), 0)
    c1 = lax.broadcasted_iota(jnp.int32, (LINES, 256), 1)
    spread = jnp.where(c0 // NK == c1 % COLS, jnp.concatenate([wide] * COLS, axis=0), 0.0)
    for part, value in zip((kron_hi, kron_lo), halves(spread)):
        part[0] = value[:, :128]
        part[1] = value[:, 128:]

    f_hi, f_lo = halves(frames_t)
    f_two = jnp.concatenate([f_hi, f_lo], axis=0)
    for r in range(ROWS):
        both_ways = dot(f_two, xhi[r], (1, 1))
        here = both_ways[:TMAX] + both_ways[TMAX:] + dot(f_hi, xlo[r], (1, 1))
        for q in range(4):
            red[q, pl.ds((r // 8) * 256 + r % 8, TMAX, stride=8), :] = here[:, 128 * q : 128 * q + 128]
    own = mine_col * 16 + mine_row
    parity = lax.rem(lax.div(mine_row, 4), 2)
    r_hi, r_lo = halves(jnp.concatenate([red[q] for q in range(4)], axis=1))
    for odd in range(2):
        t = 1 - parity if odd else parity
        twice = dot(r_hi, jnp.concatenate([kron_hi[t], kron_lo[t]], axis=1))
        core = twice[:, :128] + twice[:, 128:] + dot(r_lo, kron_hi[t])
        one, two = regroup(core[:256], core[256:])
        send1[pl.ds(32 * t, 32)] = one.reshape(32, 8, 128)
        send1[pl.ds(64 + 32 * t, 32)] = two.reshape(32, 8, 128)
        if not odd:
            recv1[own] = send1[me]
        for dx, dy, dz, dk in PEERS:
            if dx % 2 == odd:
                row, col = rows_of[dx][dy], cols_of[dz][dk]
                remote(send1.at[row * 8 + col], recv1.at[own], swap_sems.at[0], swap_sems.at[1], (row, col)).start()
    wait_for(recv1, NDEV - 1, swap_sems.at[1])

    for p in range(4):
        lanes = slice(128 * p, 128 * p + 128)
        one, two = regroup(
            recv1[32 * p : 32 * p + 16].reshape(128, 128), recv1[32 * p + 16 : 32 * p + 32].reshape(128, 128)
        )
        both_halves = [one.reshape(16, 1, 8, 128), two.reshape(16, 1, 8, 128)]
        unf_hi[:, lanes], unf_lo[:, lanes] = halves(jnp.concatenate(both_halves, axis=1).reshape(256, 128))
    pack(self_dot((unf_hi[...], unf_lo[...])), part_r)
    finish_r = all_sum(where, part_r, in_r, tot_r, sems.at[1])
    unpack(tot_r, stage, gram)
    orth(gram, brt)

    second = split_dot(halves(brt[...]), (unf_hi[...], unf_lo[...]))
    turned = second.T.reshape(8, 2, 32, RS)
    cols = [halves(turned[:, e].reshape(256, RS)) for e in range(2)]
    pack(self_dot(cols[0]) + self_dot(cols[1]), part_c)
    finish_c = all_sum(where, part_c, in_c, tot_c, sems.at[2])
    unpack(tot_c, stage, gram)
    orth(gram, bct)

    by_col, by_row = halves(bct[...].T), halves(brt[...].T)
    col_parts = halves(bct[...])
    backs = []
    for e in range(2):
        third = split_dot(col_parts, cols[e])
        backs.append(split_dot(by_col, halves(third)).reshape(8, 1, 32, RS))
    back[...] = jnp.concatenate(backs, axis=1).reshape(4, 128, RS)
    for near in (2, 1, 3, 0):
        p = where[2][near]
        pairs = split_dot(by_row, halves(back[p]), (1, 1)).reshape(16, 2, 8, 128)
        one, two = regroup(pairs[:, 0].reshape(128, 128), pairs[:, 1].reshape(128, 128))
        send2[pl.ds(32 * p, 16)] = one.reshape(16, 8, 128)
        send2[pl.ds(32 * p + 16, 16)] = two.reshape(16, 8, 128)
        if near == 0:
            recv2[me] = send2[own]
        for dx, dy, dz, dk in PEERS:
            if dz == near:
                row, col = rows_of[dx][dy], cols_of[dz][dk]
                remote(send2.at[col * 16 + row], recv2.at[me], swap_sems.at[2], swap_sems.at[3], (row, col)).start()
    wait_for(recv2, NDEV - 1, swap_sems.at[3])
    upper, lower = [], []
    for t in range(2):
        one, two = regroup(
            recv2[32 * t : 32 * t + 32].reshape(256, 128), recv2[64 + 32 * t : 96 + 32 * t].reshape(256, 128)
        )
        upper.append(one)
        lower.append(two)
    whole = jnp.concatenate([jnp.concatenate(upper, axis=1), jnp.concatenate(lower, axis=1)], axis=0)
    kron = [jnp.concatenate([part[0], part[1]], axis=1) for part in (kron_hi, kron_lo)]
    mixed = split_dot(halves(whole), kron, (1, 1))
    for q in range(4):
        mixed_out[q] = mixed[:, 128 * q : 128 * q + 128]
    for finish in (finish_f, finish_r, finish_c):
        finish()
    wait_for(send1, NDEV - 1, swap_sems.at[0])
    wait_for(send2, NDEV - 1, swap_sems.at[2])


def last_kernel(x_ref, mixed, frames, out_hbm, o_buf, store_sems):
    f_hi, f_lo = halves(frames[...])
    flat = jnp.concatenate([f_hi, f_hi, f_lo], axis=0)
    for r in range(ROWS):
        lines = pl.ds((r // 8) * 256 + r % 8, TMAX, stride=8)
        m_hi, m_lo = halves(jnp.concatenate([mixed[q, lines, :] for q in range(4)], axis=1))
        tall = jnp.concatenate([m_hi, m_lo, m_hi], axis=0)
        o_buf[r] = x_ref[r] - dot(tall, flat, (0, 0))
        pltpu.make_async_copy(o_buf.at[r], out_hbm.at[r], store_sems.at[r]).start()
    for r in range(ROWS):
        pltpu.make_async_copy(o_buf.at[r], out_hbm.at[r], store_sems.at[r]).wait()


def local(signal, start_frames, start_sends, start_rows, start_cols, rank_frames, rank_sends):
    x = signal.reshape(ROWS, LINES, NT)
    vmem = pl.BlockSpec(memory_space=pltpu.VMEM)
    smem = pl.BlockSpec(memory_space=pltpu.SMEM)
    hbm = pl.BlockSpec(memory_space=pltpu.HBM)
    tiles = lambda n: pltpu.VMEM((n, 8, 128), F32)
    flat = lambda *dims: pltpu.VMEM(dims, F32)
    short = lambda *dims: pltpu.VMEM(dims, BF16)
    held, mixed, frames = pl.pallas_call(
        main_kernel,
        out_shape=(pltpu.VMEM(x.shape, F32), pltpu.VMEM((4, 512, 128), F32), pltpu.VMEM((TMAX, NT), F32)),
        in_specs=[hbm, hbm, hbm, hbm, hbm, smem, smem],
        out_specs=(vmem, vmem, vmem),
        scratch_shapes=[
            pltpu.VMEM((ROWS, LINES, NT), BF16), pltpu.VMEM((ROWS, LINES, NT), BF16),
            flat(256, 256), flat(256, 256), flat(256, 256), flat(256, 256), flat(256, 256),
            flat(64, 6, 128), flat(64, 6, 128), flat(64, 6, 128),
            flat(NDEV - 1, 6, 128), flat(NDEV - 1, 6, 128), flat(NDEV - 1, 6, 128),
            flat(64, 6, 128), flat(64, 6, 128), flat(64, 6, 128), flat(384, 128), flat(NK, NK),
            flat(TMAX, NT), flat(KMAX, NK), flat(RS, 256), flat(RS, 256),
            flat(4, 512, 128), short(2, 512, 128), short(2, 512, 128), flat(4, 128, RS), tiles(NDEV), tiles(NDEV),
            short(256, 512), short(256, 512), tiles(NDEV), tiles(NDEV),
            pltpu.SemaphoreType.DMA((ROWS,)), pltpu.SemaphoreType.DMA((4,)), pltpu.SemaphoreType.DMA((3, 4)), pltpu.SemaphoreType.DMA((4,)),
        ],
        compiler_params=pltpu.CompilerParams(
            collective_id=1, has_side_effects=True, vmem_limit_bytes=57573376
        ),
        name="modes",
    )(x, start_frames.T, start_sends.T, start_rows.T, start_cols.T, rank_frames, rank_sends)
    out = pl.pallas_call(
        last_kernel,
        out_shape=jax.ShapeDtypeStruct(x.shape, F32),
        in_specs=[vmem, vmem, vmem],
        out_specs=pl.BlockSpec(memory_space=pl.ANY),
        scratch_shapes=[flat(ROWS, LINES, NT), pltpu.SemaphoreType.DMA((ROWS,))],
        compiler_params=pltpu.CompilerParams(vmem_limit_bytes=24 * 1024 * 1024),
        name="subtract",
    )(held, mixed, frames)
    return out.reshape(signal.shape)


def solution(mesh):
    return jax.shard_map(
        local,
        mesh=mesh,
        in_specs=(P("row", "col", None, None), P(), P(), P(), P(), P(), P()),
        out_specs=P("row", "col", None, None),
        check_vma=False,
    )
```

```python
import functools

import jax
import jax.numpy as jnp
from jax import lax
from jax.experimental import pallas as pl
from jax.experimental.pallas import tpu as pltpu
from jax.sharding import PartitionSpec as P

NT = 256
NK = 16
TMAX = 32
KMAX = 8
RS = 64
ITERS = 2
NDEV = 128
ROWS = 16
COLS = 32
LINES = COLS * NK
MESH = pl.DeviceIdType.MESH
F32 = jnp.float32
BF16 = jnp.bfloat16
HIGH = lax.Precision.HIGHEST


def me_index():
    return lax.axis_index("row") * 8 + lax.axis_index("col")


def dot(a, b, over=(1, 0)):
    dims = (((over[0],), (over[1],)), ((), ()))
    return lax.dot_general(a, b, dims, preferred_element_type=F32)


def full_dot(a, b, over=(1, 0)):
    dims = (((over[0],), (over[1],)), ((), ()))
    return lax.dot_general(a, b, dims, precision=HIGH, preferred_element_type=F32)


def halves(x):
    hi = x.astype(BF16)
    return hi, (x - hi.astype(F32)).astype(BF16)


def dot3(a, b, over=(1, 0)):
    return split_dot(halves(a), halves(b), over)


def split_dot(a, b, over=(1, 0)):
    (a_hi, a_lo), (b_hi, b_lo) = a, b
    return dot(a_hi, b_hi, over) + dot(a_hi, b_lo, over) + dot(a_lo, b_hi, over)


def self_dot(parts):
    hi, lo = parts
    side = dot(hi, lo, (1, 1))
    return dot(hi, hi, (1, 1)) + side + side.T


def remote(src, dst, send, recv, dev):
    return pltpu.make_async_remote_copy(
        src_ref=src, dst_ref=dst, send_sem=send, recv_sem=recv, device_id=dev, device_id_type=MESH
    )


def wait_for(ref, count, sem):
    some = ref.at[pl.ds(0, count)]
    pltpu.make_async_copy(some, some, sem).wait()


HOPS = (0, 1, 2, 1)
CHIPS = sorted(
    [(x, y, z) for x in range(4) for y in range(4) for z in range(4)], key=lambda o: -sum(HOPS[i] for i in o)
)
PEERS = [(x, y, z, k) for x, y, z in CHIPS for k in range(2) if x + y + z + k]


def places():
    row, col = lax.axis_index("row"), lax.axis_index("col")
    x, y, z, k = lax.div(row, 4), lax.rem(row, 4), lax.div(col, 2), lax.rem(col, 2)
    rows = [[lax.rem(x + dx, 4) * 4 + lax.rem(y + dy, 4) for dy in range(4)] for dx in range(4)]
    planes = [lax.rem(z + dz, 4) for dz in range(4)]
    cols = [[planes[dz] * 2 + lax.rem(k + dk, 2) for dk in range(2)] for dz in range(4)]
    return rows, cols, planes, k


def all_sum(where, part, inbox, total, sems):
    rows, cols, planes, k = where
    for place, (dx, dy, dz) in enumerate(CHIPS):
        row, plane = rows[dx][dy], planes[dz]
        copy = remote(
            part.at[row * 4 + plane], inbox.at[2 * place + k], sems.at[0], sems.at[1], (row, plane * 2 + 1)
        )
        if dx + dy + dz:
            copy.start()
        else:
            pl.when(k == 0)(copy.start)

    @pl.when(k == 1)
    def _():
        piece = rows[0][0] * 4 + planes[0]
        wait_for(inbox, NDEV - 1, sems.at[1])
        lanes = [inbox[i] for i in range(4)]
        for i in range(4, NDEV - 1):
            lanes[i % 4] = lanes[i % 4] + inbox[i]
        total[piece] = (lanes[0] + lanes[1]) + (lanes[2] + lanes[3]) + part[piece]
        for dx, dy, dz, dk in PEERS:
            remote(total.at[piece], total.at[piece], sems.at[2], sems.at[3], (rows[dx][dy], cols[dz][dk])).start()
        wait_for(part, 63, sems.at[3])

    @pl.when(k == 0)
    def _():
        wait_for(part, 64, sems.at[3])

    def finish():
        @pl.when(k == 1)
        def _():
            wait_for(part, 63, sems.at[0])
            wait_for(inbox, NDEV - 1, sems.at[2])

        @pl.when(k == 0)
        def _():
            wait_for(part, 64, sems.at[0])

    return finish


def pack(gram, part, extra=None):
    corner = gram[128:, 128:]
    if extra is not None:
        lane = lax.broadcasted_iota(jnp.int32, (NK, 128), 1)
        corner = jnp.concatenate([corner[: 128 - NK], jnp.where(lane < NK, extra, corner[128 - NK :])], axis=0)
    lines = jnp.concatenate([gram[:128, :128], gram[:128, 128:], corner], axis=0)
    for p in range(64):
        part[p] = lines[6 * p : 6 * p + 6]


def unpack(total, stage, gram, extra=None):
    for p in range(64):
        stage[6 * p : 6 * p + 6] = total[p]
    side = stage[128:256]
    gram[:128, :128] = stage[:128]
    gram[:128, 128:] = side
    gram[128:, :128] = side.T
    gram[128:, 128:] = stage[256:]
    if extra is not None:
        extra[...] = stage[384 - NK :, :NK]
        lane = lax.broadcasted_iota(jnp.int32, (NK, 128), 1)
        turned = stage[256:].T[128 - NK :]
        gram[256 - NK :, 128:] = jnp.where(lane < NK, turned, stage[384 - NK :])


def inverse_factor(inner, size):
    groups = size // 8
    lane = lax.broadcasted_iota(jnp.int32, (8, size), 1)
    sub = lax.broadcasted_iota(jnp.int32, (8, size), 0)
    rest = [inner[8 * g : 8 * g + 8] for g in range(groups)]
    inv = [jnp.where(lane == sub + 8 * g, 1.0, 0.0).astype(F32) for g in range(groups)]

    def row(x, j):
        return jnp.broadcast_to(x[j : j + 1], (8, size))

    def column(x, j):
        return jnp.broadcast_to(x[:, j : j + 1], (8, size))

    diag = [column(rest[0], q) for q in range(8)]
    for b in range(groups):
        below = range(b + 1, groups)
        cols = {(j, g): column(rest[g], 8 * b + j) for g in below for j in range(8)}
        ahead = [column(rest[b + 1], 8 * b + 8 + q) for q in range(8)] if below else None
        roots = jnp.ones((8, size), F32)
        for j in range(8):
            root = lax.rsqrt(row(diag[j], j))
            scale = root * root
            roots = jnp.where(sub == j, root, roots)
            heads = {q: row(diag[q], j) for q in range(j + 1, 8)}
            rest_row, inv_row = row(rest[b], j), row(inv[b], j)
            step = jnp.where(sub > j, diag[j] * scale, 0.0)
            for q in heads:
                diag[q] = diag[q] - step * heads[q]
            rest[b] = rest[b] - step * rest_row
            inv[b] = inv[b] - step * inv_row
            for g in below:
                side = cols[j, g]
                step = side * scale
                for q in heads:
                    cols[q, g] = cols[q, g] - step * heads[q]
                rest[g] = rest[g] - step * rest_row
                inv[g] = inv[g] - step * inv_row
                if g == b + 1:
                    for q in range(8):
                        ahead[q] = ahead[q] - step * row(side, q)
        inv[b] = inv[b] * roots
        diag = ahead
    return jnp.concatenate(inv, axis=0) if groups > 1 else inv[0]


def advance(image, gram, going_on):
    lower = inverse_factor(full_dot(image, image, (1, 1)), image.shape[0])
    ahead = full_dot(image, gram)
    return full_dot(lower, jnp.where(going_on, ahead, image))


def orth(*pairs):
    for gram, basis in pairs:
        basis[...] = full_dot(basis[...], gram[...])

    def step(i, c):
        values = [advance(basis[...], gram[...], i + 1 < ITERS) for gram, basis in pairs]
        for (_, basis), value in zip(pairs, values):
            basis[...] = value
        return c

    lax.fori_loop(0, ITERS, step, 0)


def swap(x):
    return pltpu.roll(x, 64, 1)


def regroup(a, b):
    left = lax.broadcasted_iota(jnp.int32, a.shape, 1) < 64
    return jnp.where(left, a, swap(b)), jnp.where(left, swap(a), b)


def main_kernel(
    x_hbm, start_f, start_s, start_r, start_c, rank_f, rank_s,
    xin, mixed_out, frames_out,
    xhi, xlo, acc, side, acc_s, side_s, gram, part_f, part_r, part_c,
    in_f, in_r, in_c, tot_f, tot_r, tot_c, stage, gram_s, bft, bst, brt, bct,
    red, kron_hi, kron_lo, back, send1, recv1, unf_hi, unf_lo, send2, recv2,
    load_sems, start_sems, sems, swap_sems,
):
    me = me_index()
    mine_row, mine_col = lax.axis_index("row"), lax.axis_index("col")
    for r in range(ROWS):
        pltpu.make_async_copy(x_hbm.at[r], xin.at[r], load_sems.at[r]).start()
    starts = [
        pltpu.make_async_copy(start, ref, start_sems.at[i])
        for i, (ref, start) in enumerate(((bft, start_f), (bst, start_s), (brt, start_r), (bct, start_c)))
    ]
    for copy in starts:
        copy.start()
    barrier = pltpu.get_barrier_semaphore()

    where = places()
    rows_of, cols_of = where[0], where[1]
    for dx, dy, dz, dk in PEERS:
        pl.semaphore_signal(barrier, inc=1, device_id=(rows_of[dx][dy], cols_of[dz][dk]), device_id_type=MESH)

    acc[...] = jnp.zeros_like(acc)
    side[...] = jnp.zeros_like(side)
    acc_s[...] = jnp.zeros_like(acc_s)
    side_s[...] = jnp.zeros_like(side_s)
    def gather(r, c):
        pltpu.make_async_copy(x_hbm.at[r], xin.at[r], load_sems.at[r]).wait()
        hi, lo = halves(xin[r])
        xhi[r] = hi
        xlo[r] = lo
        acc[...] += dot(hi, hi, (0, 0))
        side[...] += dot(hi, lo, (0, 0))
        acc_s[...] += dot(hi[:256], hi[:256], (1, 1)) + dot(hi[256:], hi[256:], (1, 1))
        side_s[...] += dot(hi[:256], lo[:256], (1, 1)) + dot(hi[256:], lo[256:], (1, 1))
        return c

    lax.fori_loop(0, ROWS, gather, 0)
    sends = acc_s[...] + side_s[...] + side_s[...].T
    i0 = lax.broadcasted_iota(jnp.int32, (256, 256), 0)
    i1 = lax.broadcasted_iota(jnp.int32, (256, 256), 1)
    sends = jnp.where(i0 // NK == i1 // NK, sends, 0.0).reshape(16, NK, 256).sum(axis=0)
    j0 = lax.broadcasted_iota(jnp.int32, (256, 128), 0)
    j1 = lax.broadcasted_iota(jnp.int32, (256, 128), 1)
    small = full_dot(sends, (j0 % NK == j1).astype(F32))
    pack(acc[...] + side[...] + side[...].T, part_f, small)

    for copy in starts:
        copy.wait()
    pl.semaphore_wait(barrier, NDEV - 1)
    finish_f = all_sum(where, part_f, in_f, tot_f, sems.at[0])

    unpack(tot_f, stage, gram, gram_s)

    orth((gram, bft), (gram_s, bst))
    keep_f = lax.broadcasted_iota(jnp.int32, (TMAX, NT), 0) < rank_f[0]
    frames_t = bft[...] * keep_f.astype(F32)
    frames_out[...] = frames_t
    keep_s = lax.broadcasted_iota(jnp.int32, (KMAX, NK), 0) < rank_s[0]
    sends = bst[...] * keep_s.astype(F32)
    a0 = lax.broadcasted_iota(jnp.int32, (KMAX, 256), 0)
    a1 = lax.broadcasted_iota(jnp.int32, (KMAX, 256), 1)
    wide = full_dot(sends, (a0 == a1 // COLS).astype(F32), (0, 0))
    c0 = lax.broadcasted_iota(jnp.int32, (LINES, 256), 0)
    c1 = lax.broadcasted_iota(jnp.int32, (LINES, 256), 1)
    spread = jnp.where(c0 // NK == c1 % COLS, jnp.concatenate([wide] * COLS, axis=0), 0.0)
    for part, value in zip((kron_hi, kron_lo), halves(spread)):
        part[0] = value[:, :128]
        part[1] = value[:, 128:]

    f_hi, f_lo = halves(frames_t)
    f_two = jnp.concatenate([f_hi, f_lo], axis=0)
    for r in range(ROWS):
        both_ways = dot(f_two, xhi[r], (1, 1))
        here = both_ways[:TMAX] + both_ways[TMAX:] + dot(f_hi, xlo[r], (1, 1))
        for q in range(4):
            red[q, pl.ds((r // 8) * 256 + r % 8, TMAX, stride=8), :] = here[:, 128 * q : 128 * q + 128]
    own = mine_col * 16 + mine_row
    parity = lax.rem(lax.div(mine_row, 4), 2)
    r_hi, r_lo = halves(jnp.concatenate([red[q] for q in range(4)], axis=1))
    for odd in range(2):
        t = 1 - parity if odd else parity
        twice = dot(r_hi, jnp.concatenate([kron_hi[t], kron_lo[t]], axis=1))
        core = twice[:, :128] + twice[:, 128:] + dot(r_lo, kron_hi[t])
        one, two = regroup(core[:256], core[256:])
        send1[pl.ds(32 * t, 32)] = one.reshape(32, 8, 128)
        send1[pl.ds(64 + 32 * t, 32)] = two.reshape(32, 8, 128)
        if not odd:
            recv1[own] = send1[me]
        for dx, dy, dz, dk in PEERS:
            if dx % 2 == odd:
                row, col = rows_of[dx][dy], cols_of[dz][dk]
                remote(send1.at[row * 8 + col], recv1.at[own], swap_sems.at[0], swap_sems.at[1], (row, col)).start()
    wait_for(recv1, NDEV - 1, swap_sems.at[1])

    for p in range(4):
        lanes = slice(128 * p, 128 * p + 128)
        one, two = regroup(
            recv1[32 * p : 32 * p + 16].reshape(128, 128), recv1[32 * p + 16 : 32 * p + 32].reshape(128, 128)
        )
        both_halves = [one.reshape(16, 1, 8, 128), two.reshape(16, 1, 8, 128)]
        unf_hi[:, lanes], unf_lo[:, lanes] = halves(jnp.concatenate(both_halves, axis=1).reshape(256, 128))
    pack(self_dot((unf_hi[...], unf_lo[...])), part_r)
    finish_r = all_sum(where, part_r, in_r, tot_r, sems.at[1])
    unpack(tot_r, stage, gram)
    orth((gram, brt))

    second = split_dot(halves(brt[...]), (unf_hi[...], unf_lo[...]))
    turned = second.T.reshape(8, 2, 32, RS)
    cols = [halves(turned[:, e].reshape(256, RS)) for e in range(2)]
    pack(self_dot(cols[0]) + self_dot(cols[1]), part_c)
    finish_c = all_sum(where, part_c, in_c, tot_c, sems.at[2])
    unpack(tot_c, stage, gram)
    orth((gram, bct))

    by_col, by_row = halves(bct[...].T), halves(brt[...].T)
    col_parts = halves(bct[...])
    backs = []
    for e in range(2):
        third = split_dot(col_parts, cols[e])
        backs.append(split_dot(by_col, halves(third)).reshape(8, 1, 32, RS))
    back[...] = jnp.concatenate(backs, axis=1).reshape(4, 128, RS)
    for near in (2, 1, 3, 0):
        p = where[2][near]
        pairs = split_dot(by_row, halves(back[p]), (1, 1)).reshape(16, 2, 8, 128)
        one, two = regroup(pairs[:, 0].reshape(128, 128), pairs[:, 1].reshape(128, 128))
        send2[pl.ds(32 * p, 16)] = one.reshape(16, 8, 128)
        send2[pl.ds(32 * p + 16, 16)] = two.reshape(16, 8, 128)
        if near == 0:
            recv2[me] = send2[own]
        for dx, dy, dz, dk in PEERS:
            if dz == near:
                row, col = rows_of[dx][dy], cols_of[dz][dk]
                remote(send2.at[col * 16 + row], recv2.at[me], swap_sems.at[2], swap_sems.at[3], (row, col)).start()
    wait_for(recv2, NDEV - 1, swap_sems.at[3])
    upper, lower = [], []
    for t in range(2):
        one, two = regroup(
            recv2[32 * t : 32 * t + 32].reshape(256, 128), recv2[64 + 32 * t : 96 + 32 * t].reshape(256, 128)
        )
        upper.append(one)
        lower.append(two)
    whole = jnp.concatenate([jnp.concatenate(upper, axis=1), jnp.concatenate(lower, axis=1)], axis=0)
    kron = [jnp.concatenate([part[0], part[1]], axis=1) for part in (kron_hi, kron_lo)]
    mixed = split_dot(halves(whole), kron, (1, 1))
    for q in range(4):
        mixed_out[q] = mixed[:, 128 * q : 128 * q + 128]
    for finish in (finish_f, finish_r, finish_c):
        finish()
    wait_for(send1, NDEV - 1, swap_sems.at[0])
    wait_for(send2, NDEV - 1, swap_sems.at[2])


def last_kernel(x_ref, mixed, frames, out_hbm, o_buf, store_sems):
    f_hi, f_lo = halves(frames[...])
    flat = jnp.concatenate([f_hi, f_hi, f_lo], axis=0)
    for r in range(ROWS):
        lines = pl.ds((r // 8) * 256 + r % 8, TMAX, stride=8)
        m_hi, m_lo = halves(jnp.concatenate([mixed[q, lines, :] for q in range(4)], axis=1))
        tall = jnp.concatenate([m_hi, m_lo, m_hi], axis=0)
        o_buf[r] = x_ref[r] - dot(tall, flat, (0, 0))
        pltpu.make_async_copy(o_buf.at[r], out_hbm.at[r], store_sems.at[r]).start()
    for r in range(ROWS):
        pltpu.make_async_copy(o_buf.at[r], out_hbm.at[r], store_sems.at[r]).wait()


def local(signal, start_frames, start_sends, start_rows, start_cols, rank_frames, rank_sends):
    x = signal.reshape(ROWS, LINES, NT)
    vmem = pl.BlockSpec(memory_space=pltpu.VMEM)
    smem = pl.BlockSpec(memory_space=pltpu.SMEM)
    hbm = pl.BlockSpec(memory_space=pltpu.HBM)
    tiles = lambda n: pltpu.VMEM((n, 8, 128), F32)
    flat = lambda *dims: pltpu.VMEM(dims, F32)
    short = lambda *dims: pltpu.VMEM(dims, BF16)
    held, mixed, frames = pl.pallas_call(
        main_kernel,
        out_shape=(pltpu.VMEM(x.shape, F32), pltpu.VMEM((4, 512, 128), F32), pltpu.VMEM((TMAX, NT), F32)),
        in_specs=[hbm, hbm, hbm, hbm, hbm, smem, smem],
        out_specs=(vmem, vmem, vmem),
        scratch_shapes=[
            pltpu.VMEM((ROWS, LINES, NT), BF16), pltpu.VMEM((ROWS, LINES, NT), BF16),
            flat(256, 256), flat(256, 256), flat(256, 256), flat(256, 256), flat(256, 256),
            flat(64, 6, 128), flat(64, 6, 128), flat(64, 6, 128),
            flat(NDEV - 1, 6, 128), flat(NDEV - 1, 6, 128), flat(NDEV - 1, 6, 128),
            flat(64, 6, 128), flat(64, 6, 128), flat(64, 6, 128), flat(384, 128), flat(NK, NK),
            flat(TMAX, NT), flat(KMAX, NK), flat(RS, 256), flat(RS, 256),
            flat(4, 512, 128), short(2, 512, 128), short(2, 512, 128), flat(4, 128, RS), tiles(NDEV), tiles(NDEV),
            short(256, 512), short(256, 512), tiles(NDEV), tiles(NDEV),
            pltpu.SemaphoreType.DMA((ROWS,)), pltpu.SemaphoreType.DMA((4,)), pltpu.SemaphoreType.DMA((3, 4)), pltpu.SemaphoreType.DMA((4,)),
        ],
        compiler_params=pltpu.CompilerParams(
            collective_id=1, has_side_effects=True, vmem_limit_bytes=57573376
        ),
        name="modes",
    )(x, start_frames.T, start_sends.T, start_rows.T, start_cols.T, rank_frames, rank_sends)
    out = pl.pallas_call(
        last_kernel,
        out_shape=jax.ShapeDtypeStruct(x.shape, F32),
        in_specs=[vmem, vmem, vmem],
        out_specs=pl.BlockSpec(memory_space=pl.ANY),
        scratch_shapes=[flat(ROWS, LINES, NT), pltpu.SemaphoreType.DMA((ROWS,))],
        compiler_params=pltpu.CompilerParams(vmem_limit_bytes=24 * 1024 * 1024),
        name="subtract",
    )(held, mixed, frames)
    return out.reshape(signal.shape)


def solution(mesh):
    return jax.shard_map(
        local,
        mesh=mesh,
        in_specs=(P("row", "col", None, None), P(), P(), P(), P(), P(), P()),
        out_specs=P("row", "col", None, None),
        check_vma=False,
    )
```

```python
import functools

import jax
import jax.numpy as jnp
from jax import lax
from jax.experimental import pallas as pl
from jax.experimental.pallas import tpu as pltpu
from jax.sharding import PartitionSpec as P

NT = 256
NK = 16
TMAX = 32
KMAX = 8
RS = 64
ITERS = 2
NDEV = 128
ROWS = 16
COLS = 32
LINES = COLS * NK
MESH = pl.DeviceIdType.MESH
F32 = jnp.float32
BF16 = jnp.bfloat16
HIGH = lax.Precision.HIGHEST


def me_index():
    return lax.axis_index("row") * 8 + lax.axis_index("col")


def dot(a, b, over=(1, 0)):
    dims = (((over[0],), (over[1],)), ((), ()))
    return lax.dot_general(a, b, dims, preferred_element_type=F32)


def full_dot(a, b, over=(1, 0)):
    dims = (((over[0],), (over[1],)), ((), ()))
    return lax.dot_general(a, b, dims, precision=HIGH, preferred_element_type=F32)


def halves(x):
    hi = x.astype(BF16)
    return hi, (x - hi.astype(F32)).astype(BF16)


def dot3(a, b, over=(1, 0)):
    return split_dot(halves(a), halves(b), over)


def split_dot(a, b, over=(1, 0)):
    (a_hi, a_lo), (b_hi, b_lo) = a, b
    return dot(a_hi, b_hi, over) + dot(a_hi, b_lo, over) + dot(a_lo, b_hi, over)


def self_dot(parts):
    hi, lo = parts
    side = dot(hi, lo, (1, 1))
    return dot(hi, hi, (1, 1)) + side + side.T


def remote(src, dst, send, recv, dev):
    return pltpu.make_async_remote_copy(
        src_ref=src, dst_ref=dst, send_sem=send, recv_sem=recv, device_id=dev, device_id_type=MESH
    )


def wait_for(ref, count, sem):
    some = ref.at[pl.ds(0, count)]
    pltpu.make_async_copy(some, some, sem).wait()


HOPS = (0, 1, 2, 1)
CHIPS = sorted(
    [(x, y, z) for x in range(4) for y in range(4) for z in range(4)], key=lambda o: -sum(HOPS[i] for i in o)
)
PEERS = [(x, y, z, k) for x, y, z in CHIPS for k in range(2) if x + y + z + k]


def places():
    row, col = lax.axis_index("row"), lax.axis_index("col")
    x, y, z, k = lax.div(row, 4), lax.rem(row, 4), lax.div(col, 2), lax.rem(col, 2)
    rows = [[lax.rem(x + dx, 4) * 4 + lax.rem(y + dy, 4) for dy in range(4)] for dx in range(4)]
    planes = [lax.rem(z + dz, 4) for dz in range(4)]
    cols = [[planes[dz] * 2 + lax.rem(k + dk, 2) for dk in range(2)] for dz in range(4)]
    return rows, cols, planes, k


def all_sum(where, part, inbox, total, sems):
    rows, cols, planes, k = where
    for place, (dx, dy, dz) in enumerate(CHIPS):
        row, plane = rows[dx][dy], planes[dz]
        slot = 2 * place + k if dx + dy + dz else 2 * place
        copy = remote(
            part.at[row * 4 + plane], inbox.at[slot], sems.at[0], sems.at[1], (row, plane * 2 + 1)
        )
        if dx + dy + dz:
            copy.start()
        else:
            pl.when(k == 0)(copy.start)

    @pl.when(k == 1)
    def _():
        piece = rows[0][0] * 4 + planes[0]
        wait_for(inbox, NDEV - 1, sems.at[1])
        lanes = [inbox[i] for i in range(4)]
        for i in range(4, NDEV - 1):
            lanes[i % 4] = lanes[i % 4] + inbox[i]
        total[piece] = (lanes[0] + lanes[1]) + (lanes[2] + lanes[3]) + part[piece]
        for dx, dy, dz, dk in PEERS:
            remote(total.at[piece], total.at[piece], sems.at[2], sems.at[3], (rows[dx][dy], cols[dz][dk])).start()
        wait_for(part, 63, sems.at[3])

    @pl.when(k == 0)
    def _():
        wait_for(part, 64, sems.at[3])

    def finish():
        @pl.when(k == 1)
        def _():
            wait_for(part, 63, sems.at[0])
            wait_for(inbox, NDEV - 1, sems.at[2])

        @pl.when(k == 0)
        def _():
            wait_for(part, 64, sems.at[0])

    return finish


def pack(gram, part, extra=None):
    corner = gram[128:, 128:]
    if extra is not None:
        lane = lax.broadcasted_iota(jnp.int32, (NK, 128), 1)
        corner = jnp.concatenate([corner[: 128 - NK], jnp.where(lane < NK, extra, corner[128 - NK :])], axis=0)
    lines = jnp.concatenate([gram[:128, :128], gram[:128, 128:], corner], axis=0)
    for p in range(64):
        part[p] = lines[6 * p : 6 * p + 6]


def unpack(total, stage, gram, extra=None):
    for p in range(64):
        stage[6 * p : 6 * p + 6] = total[p]
    side = stage[128:256]
    gram[:128, :128] = stage[:128]
    gram[:128, 128:] = side
    gram[128:, :128] = side.T
    gram[128:, 128:] = stage[256:]
    if extra is not None:
        extra[...] = stage[384 - NK :, :NK]
        lane = lax.broadcasted_iota(jnp.int32, (NK, 128), 1)
        turned = stage[256:].T[128 - NK :]
        gram[256 - NK :, 128:] = jnp.where(lane < NK, turned, stage[384 - NK :])


def inverse_factor(inner, size):
    groups = size // 8
    lane = lax.broadcasted_iota(jnp.int32, (8, size), 1)
    sub = lax.broadcasted_iota(jnp.int32, (8, size), 0)
    rest = [inner[8 * g : 8 * g + 8] for g in range(groups)]
    inv = [jnp.where(lane == sub + 8 * g, 1.0, 0.0).astype(F32) for g in range(groups)]

    def row(x, j):
        return jnp.broadcast_to(x[j : j + 1], (8, size))

    def column(x, j):
        return jnp.broadcast_to(x[:, j : j + 1], (8, size))

    diag = [column(rest[0], q) for q in range(8)]
    for b in range(groups):
        below = range(b + 1, groups)
        cols = {(j, g): column(rest[g], 8 * b + j) for g in below for j in range(8)}
        ahead = [column(rest[b + 1], 8 * b + 8 + q) for q in range(8)] if below else None
        roots = jnp.ones((8, size), F32)
        for j in range(8):
            root = lax.rsqrt(row(diag[j], j))
            scale = root * root
            roots = jnp.where(sub == j, root, roots)
            heads = {q: row(diag[q], j) for q in range(j + 1, 8)}
            rest_row, inv_row = row(rest[b], j), row(inv[b], j)
            step = jnp.where(sub > j, diag[j] * scale, 0.0)
            for q in heads:
                diag[q] = diag[q] - step * heads[q]
            rest[b] = rest[b] - step * rest_row
            inv[b] = inv[b] - step * inv_row
            for g in below:
                side = cols[j, g]
                step = side * scale
                for q in heads:
                    cols[q, g] = cols[q, g] - step * heads[q]
                rest[g] = rest[g] - step * rest_row
                inv[g] = inv[g] - step * inv_row
                if g == b + 1:
                    for q in range(8):
                        ahead[q] = ahead[q] - step * row(side, q)
        inv[b] = inv[b] * roots
        diag = ahead
    return jnp.concatenate(inv, axis=0) if groups > 1 else inv[0]


def advance(image, gram, going_on):
    lower = inverse_factor(full_dot(image, image, (1, 1)), image.shape[0])
    ahead = full_dot(image, gram)
    return full_dot(lower, jnp.where(going_on, ahead, image))


def orth(*pairs):
    for gram, basis in pairs:
        basis[...] = full_dot(basis[...], gram[...])

    def step(i, c):
        values = [advance(basis[...], gram[...], i + 1 < ITERS) for gram, basis in pairs]
        for (_, basis), value in zip(pairs, values):
            basis[...] = value
        return c

    lax.fori_loop(0, ITERS, step, 0)


def swap(x):
    return pltpu.roll(x, 64, 1)


def regroup(a, b):
    left = lax.broadcasted_iota(jnp.int32, a.shape, 1) < 64
    return jnp.where(left, a, swap(b)), jnp.where(left, swap(a), b)


def main_kernel(
    x_hbm, start_f, start_s, start_r, start_c, rank_f, rank_s,
    xin, mixed_out, frames_out,
    xhi, xlo, acc, side, acc_s, gram, part_f, part_r, part_c,
    in_f, in_r, in_c, tot_f, tot_r, tot_c, stage, gram_s, bft, bst, brt, bct,
    red, kron_hi, kron_lo, back, send1, recv1, unf_hi, unf_lo, send2, recv2,
    load_sems, start_sems, sems, swap_sems,
):
    me = me_index()
    mine_row, mine_col = lax.axis_index("row"), lax.axis_index("col")
    for r in range(ROWS):
        pltpu.make_async_copy(x_hbm.at[r], xin.at[r], load_sems.at[r]).start()
    starts = [
        pltpu.make_async_copy(start, ref, start_sems.at[i])
        for i, (ref, start) in enumerate(((bft, start_f), (bst, start_s), (brt, start_r), (bct, start_c)))
    ]
    for copy in starts:
        copy.start()
    barrier = pltpu.get_barrier_semaphore()

    where = places()
    rows_of, cols_of = where[0], where[1]
    for dx, dy, dz, dk in PEERS:
        pl.semaphore_signal(barrier, inc=1, device_id=(rows_of[dx][dy], cols_of[dz][dk]), device_id_type=MESH)

    acc[...] = jnp.zeros_like(acc)
    side[...] = jnp.zeros_like(side)
    acc_s[...] = jnp.zeros_like(acc_s)
    def gather(r, c):
        pltpu.make_async_copy(x_hbm.at[r], xin.at[r], load_sems.at[r]).wait()
        hi, lo = halves(xin[r])
        xhi[r] = hi
        xlo[r] = lo
        acc[...] += dot(hi, hi, (0, 0))
        side[...] += dot(hi, lo, (0, 0))
        block = 0.0
        for q in range(0, LINES, 128):
            here = hi[q : q + 128]
            block += dot(here, jnp.concatenate([here, lo[q : q + 128]], axis=0), (1, 1))
        acc_s[...] += block
        return c

    lax.fori_loop(0, ROWS, gather, 0)
    mixed_in = acc_s[:, 128:]
    sends = acc_s[:, :128] + mixed_in + mixed_in.T
    j0 = lax.broadcasted_iota(jnp.int32, (128, 128), 0)
    j1 = lax.broadcasted_iota(jnp.int32, (128, 128), 1)
    sends = jnp.where(j0 // NK == j1 // NK, sends, 0.0).reshape(8, NK, 128).sum(axis=0)
    small = full_dot(sends, (j0 % NK == j1).astype(F32))
    pack(acc[...] + side[...] + side[...].T, part_f, small)

    for copy in starts:
        copy.wait()
    pl.semaphore_wait(barrier, NDEV - 1)
    finish_f = all_sum(where, part_f, in_f, tot_f, sems.at[0])

    unpack(tot_f, stage, gram, gram_s)

    orth((gram, bft), (gram_s, bst))
    keep_f = lax.broadcasted_iota(jnp.int32, (TMAX, NT), 0) < rank_f[0]
    frames_t = bft[...] * keep_f.astype(F32)
    frames_out[...] = frames_t
    keep_s = lax.broadcasted_iota(jnp.int32, (KMAX, NK), 0) < rank_s[0]
    sends = bst[...] * keep_s.astype(F32)
    a0 = lax.broadcasted_iota(jnp.int32, (KMAX, 256), 0)
    a1 = lax.broadcasted_iota(jnp.int32, (KMAX, 256), 1)
    wide = full_dot(sends, (a0 == a1 // COLS).astype(F32), (0, 0))
    c0 = lax.broadcasted_iota(jnp.int32, (LINES, 256), 0)
    c1 = lax.broadcasted_iota(jnp.int32, (LINES, 256), 1)
    spread = jnp.where(c0 // NK == c1 % COLS, jnp.concatenate([wide] * COLS, axis=0), 0.0)
    for part, value in zip((kron_hi, kron_lo), halves(spread)):
        part[0] = value[:, :128]
        part[1] = value[:, 128:]

    f_hi, f_lo = halves(frames_t)
    f_two = jnp.concatenate([f_hi, f_lo], axis=0)
    for r in range(ROWS):
        both_ways = dot(f_two, xhi[r], (1, 1))
        here = both_ways[:TMAX] + both_ways[TMAX:] + dot(f_hi, xlo[r], (1, 1))
        for q in range(4):
            red[q, pl.ds((r // 8) * 256 + r % 8, TMAX, stride=8), :] = here[:, 128 * q : 128 * q + 128]
    own = mine_col * 16 + mine_row
    parity = lax.rem(lax.div(mine_row, 4), 2)
    r_hi, r_lo = halves(jnp.concatenate([red[q] for q in range(4)], axis=1))
    for odd in range(2):
        t = 1 - parity if odd else parity
        twice = dot(r_hi, jnp.concatenate([kron_hi[t], kron_lo[t]], axis=1))
        core = twice[:, :128] + twice[:, 128:] + dot(r_lo, kron_hi[t])
        one, two = regroup(core[:256], core[256:])
        send1[pl.ds(32 * t, 32)] = one.reshape(32, 8, 128)
        send1[pl.ds(64 + 32 * t, 32)] = two.reshape(32, 8, 128)
        if not odd:
            recv1[own] = send1[me]
        for dx, dy, dz, dk in PEERS:
            if dx % 2 == odd:
                row, col = rows_of[dx][dy], cols_of[dz][dk]
                remote(send1.at[row * 8 + col], recv1.at[own], swap_sems.at[0], swap_sems.at[1], (row, col)).start()
    wait_for(recv1, NDEV - 1, swap_sems.at[1])

    for p in range(4):
        lanes = slice(128 * p, 128 * p + 128)
        one, two = regroup(
            recv1[32 * p : 32 * p + 16].reshape(128, 128), recv1[32 * p + 16 : 32 * p + 32].reshape(128, 128)
        )
        both_halves = [one.reshape(16, 1, 8, 128), two.reshape(16, 1, 8, 128)]
        unf_hi[:, lanes], unf_lo[:, lanes] = halves(jnp.concatenate(both_halves, axis=1).reshape(256, 128))
    pack(self_dot((unf_hi[...], unf_lo[...])), part_r)
    finish_r = all_sum(where, part_r, in_r, tot_r, sems.at[1])
    unpack(tot_r, stage, gram)
    orth((gram, brt))

    second = split_dot(halves(brt[...]), (unf_hi[...], unf_lo[...]))
    turned = second.T.reshape(8, 2, 32, RS)
    cols = [halves(turned[:, e].reshape(256, RS)) for e in range(2)]
    pack(self_dot(cols[0]) + self_dot(cols[1]), part_c)
    finish_c = all_sum(where, part_c, in_c, tot_c, sems.at[2])
    unpack(tot_c, stage, gram)
    orth((gram, bct))

    by_col, by_row = halves(bct[...].T), halves(brt[...].T)
    col_parts = halves(bct[...])
    backs = []
    for e in range(2):
        third = split_dot(col_parts, cols[e])
        backs.append(split_dot(by_col, halves(third)).reshape(8, 1, 32, RS))
    back[...] = jnp.concatenate(backs, axis=1).reshape(4, 128, RS)
    for near in (2, 1, 3, 0):
        p = where[2][near]
        pairs = split_dot(by_row, halves(back[p]), (1, 1)).reshape(16, 2, 8, 128)
        one, two = regroup(pairs[:, 0].reshape(128, 128), pairs[:, 1].reshape(128, 128))
        send2[pl.ds(32 * p, 16)] = one.reshape(16, 8, 128)
        send2[pl.ds(32 * p + 16, 16)] = two.reshape(16, 8, 128)
        if near == 0:
            recv2[me] = send2[own]
        for dx, dy, dz, dk in PEERS:
            if dz == near:
                row, col = rows_of[dx][dy], cols_of[dz][dk]
                remote(send2.at[col * 16 + row], recv2.at[me], swap_sems.at[2], swap_sems.at[3], (row, col)).start()
    wait_for(recv2, NDEV - 1, swap_sems.at[3])
    upper, lower = [], []
    for t in range(2):
        one, two = regroup(
            recv2[32 * t : 32 * t + 32].reshape(256, 128), recv2[64 + 32 * t : 96 + 32 * t].reshape(256, 128)
        )
        upper.append(one)
        lower.append(two)
    whole = jnp.concatenate([jnp.concatenate(upper, axis=1), jnp.concatenate(lower, axis=1)], axis=0)
    kron = [jnp.concatenate([part[0], part[1]], axis=1) for part in (kron_hi, kron_lo)]
    mixed = split_dot(halves(whole), kron, (1, 1))
    for q in range(4):
        mixed_out[q] = mixed[:, 128 * q : 128 * q + 128]
    for finish in (finish_f, finish_r, finish_c):
        finish()
    wait_for(send1, NDEV - 1, swap_sems.at[0])
    wait_for(send2, NDEV - 1, swap_sems.at[2])


def last_kernel(x_ref, mixed, frames, out_hbm, o_buf, store_sems):
    f_hi, f_lo = halves(frames[...])
    flat = jnp.concatenate([f_hi, f_hi, f_lo], axis=0)
    for r in range(ROWS):
        lines = pl.ds((r // 8) * 256 + r % 8, TMAX, stride=8)
        m_hi, m_lo = halves(jnp.concatenate([mixed[q, lines, :] for q in range(4)], axis=1))
        tall = jnp.concatenate([m_hi, m_lo, m_hi], axis=0)
        o_buf[r] = x_ref[r] - dot(tall, flat, (0, 0))
        pltpu.make_async_copy(o_buf.at[r], out_hbm.at[r], store_sems.at[r]).start()
    for r in range(ROWS):
        pltpu.make_async_copy(o_buf.at[r], out_hbm.at[r], store_sems.at[r]).wait()


def local(signal, start_frames, start_sends, start_rows, start_cols, rank_frames, rank_sends):
    x = signal.reshape(ROWS, LINES, NT)
    vmem = pl.BlockSpec(memory_space=pltpu.VMEM)
    smem = pl.BlockSpec(memory_space=pltpu.SMEM)
    hbm = pl.BlockSpec(memory_space=pltpu.HBM)
    tiles = lambda n: pltpu.VMEM((n, 8, 128), F32)
    flat = lambda *dims: pltpu.VMEM(dims, F32)
    short = lambda *dims: pltpu.VMEM(dims, BF16)
    held, mixed, frames = pl.pallas_call(
        main_kernel,
        out_shape=(pltpu.VMEM(x.shape, F32), pltpu.VMEM((4, 512, 128), F32), pltpu.VMEM((TMAX, NT), F32)),
        in_specs=[hbm, hbm, hbm, hbm, hbm, smem, smem],
        out_specs=(vmem, vmem, vmem),
        scratch_shapes=[
            pltpu.VMEM((ROWS, LINES, NT), BF16), pltpu.VMEM((ROWS, LINES, NT), BF16),
            flat(256, 256), flat(256, 256), flat(128, 256), flat(256, 256),
            flat(64, 6, 128), flat(64, 6, 128), flat(64, 6, 128),
            flat(NDEV - 1, 6, 128), flat(NDEV - 1, 6, 128), flat(NDEV - 1, 6, 128),
            flat(64, 6, 128), flat(64, 6, 128), flat(64, 6, 128), flat(384, 128), flat(NK, NK),
            flat(TMAX, NT), flat(KMAX, NK), flat(RS, 256), flat(RS, 256),
            flat(4, 512, 128), short(2, 512, 128), short(2, 512, 128), flat(4, 128, RS), tiles(NDEV), tiles(NDEV),
            short(256, 512), short(256, 512), tiles(NDEV), tiles(NDEV),
            pltpu.SemaphoreType.DMA((ROWS,)), pltpu.SemaphoreType.DMA((4,)), pltpu.SemaphoreType.DMA((3, 4)), pltpu.SemaphoreType.DMA((4,)),
        ],
        compiler_params=pltpu.CompilerParams(
            collective_id=1, has_side_effects=True, vmem_limit_bytes=57573376
        ),
        name="modes",
    )(x, start_frames.T, start_sends.T, start_rows.T, start_cols.T, rank_frames, rank_sends)
    out = pl.pallas_call(
        last_kernel,
        out_shape=jax.ShapeDtypeStruct(x.shape, F32),
        in_specs=[vmem, vmem, vmem],
        out_specs=pl.BlockSpec(memory_space=pl.ANY),
        scratch_shapes=[flat(ROWS, LINES, NT), pltpu.SemaphoreType.DMA((ROWS,))],
        compiler_params=pltpu.CompilerParams(vmem_limit_bytes=24 * 1024 * 1024),
        name="subtract",
    )(held, mixed, frames)
    return out.reshape(signal.shape)


def solution(mesh):
    return jax.shard_map(
        local,
        mesh=mesh,
        in_specs=(P("row", "col", None, None), P(), P(), P(), P(), P(), P()),
        out_specs=P("row", "col", None, None),
        check_vma=False,
    )
```

```python
import functools

import jax
import jax.numpy as jnp
from jax import lax
from jax.experimental import pallas as pl
from jax.experimental.pallas import tpu as pltpu
from jax.sharding import PartitionSpec as P

NT = 256
NK = 16
TMAX = 32
KMAX = 8
RS = 64
ITERS = 2
NDEV = 128
ROWS = 16
COLS = 32
LINES = COLS * NK
MESH = pl.DeviceIdType.MESH
F32 = jnp.float32
BF16 = jnp.bfloat16
HIGH = lax.Precision.HIGHEST


def me_index():
    return lax.axis_index("row") * 8 + lax.axis_index("col")


def dot(a, b, over=(1, 0)):
    dims = (((over[0],), (over[1],)), ((), ()))
    return lax.dot_general(a, b, dims, preferred_element_type=F32)


def full_dot(a, b, over=(1, 0)):
    dims = (((over[0],), (over[1],)), ((), ()))
    return lax.dot_general(a, b, dims, precision=HIGH, preferred_element_type=F32)


def halves(x):
    hi = x.astype(BF16)
    return hi, (x - hi.astype(F32)).astype(BF16)


def dot3(a, b, over=(1, 0)):
    return split_dot(halves(a), halves(b), over)


def split_dot(a, b, over=(1, 0)):
    (a_hi, a_lo), (b_hi, b_lo) = a, b
    return dot(a_hi, b_hi, over) + dot(a_hi, b_lo, over) + dot(a_lo, b_hi, over)


def self_dot(parts):
    hi, lo = parts
    side = dot(hi, lo, (1, 1))
    return dot(hi, hi, (1, 1)) + side + side.T


def remote(src, dst, send, recv, dev):
    return pltpu.make_async_remote_copy(
        src_ref=src, dst_ref=dst, send_sem=send, recv_sem=recv, device_id=dev, device_id_type=MESH
    )


def wait_for(ref, count, sem):
    some = ref.at[pl.ds(0, count)]
    pltpu.make_async_copy(some, some, sem).wait()


HOPS = (0, 1, 2, 1)
CHIPS = sorted(
    [(x, y, z) for x in range(4) for y in range(4) for z in range(4)], key=lambda o: -sum(HOPS[i] for i in o)
)
PEERS = [(x, y, z, k) for x, y, z in CHIPS for k in range(2) if x + y + z + k]


def places():
    row, col = lax.axis_index("row"), lax.axis_index("col")
    x, y, z, k = lax.div(row, 4), lax.rem(row, 4), lax.div(col, 2), lax.rem(col, 2)
    rows = [[lax.rem(x + dx, 4) * 4 + lax.rem(y + dy, 4) for dy in range(4)] for dx in range(4)]
    planes = [lax.rem(z + dz, 4) for dz in range(4)]
    cols = [[planes[dz] * 2 + lax.rem(k + dk, 2) for dk in range(2)] for dz in range(4)]
    return rows, cols, planes, k


def all_sum(where, part, inbox, total, sems):
    rows, cols, planes, k = where
    for place, (dx, dy, dz) in enumerate(CHIPS):
        row, plane = rows[dx][dy], planes[dz]
        slot = 2 * place + k if dx + dy + dz else 2 * place
        copy = remote(
            part.at[row * 4 + plane], inbox.at[slot], sems.at[0], sems.at[1], (row, plane * 2 + 1)
        )
        if dx + dy + dz:
            copy.start()
        else:
            pl.when(k == 0)(copy.start)

    @pl.when(k == 1)
    def _():
        piece = rows[0][0] * 4 + planes[0]
        wait_for(inbox, NDEV - 1, sems.at[1])
        lanes = [inbox[i] for i in range(4)]
        for i in range(4, NDEV - 1):
            lanes[i % 4] = lanes[i % 4] + inbox[i]
        total[piece] = (lanes[0] + lanes[1]) + (lanes[2] + lanes[3]) + part[piece]
        for dx, dy, dz, dk in PEERS:
            remote(total.at[piece], total.at[piece], sems.at[2], sems.at[3], (rows[dx][dy], cols[dz][dk])).start()
        wait_for(part, 63, sems.at[3])

    @pl.when(k == 0)
    def _():
        wait_for(part, 64, sems.at[3])

    def finish():
        @pl.when(k == 1)
        def _():
            wait_for(part, 63, sems.at[0])
            wait_for(inbox, NDEV - 1, sems.at[2])

        @pl.when(k == 0)
        def _():
            wait_for(part, 64, sems.at[0])

    return finish


def pack(gram, part, extra=None):
    corner = gram[128:, 128:]
    if extra is not None:
        lane = lax.broadcasted_iota(jnp.int32, (NK, 128), 1)
        corner = jnp.concatenate([corner[: 128 - NK], jnp.where(lane < NK, extra, corner[128 - NK :])], axis=0)
    lines = jnp.concatenate([gram[:128, :128], gram[:128, 128:], corner], axis=0)
    for p in range(64):
        part[p] = lines[6 * p : 6 * p + 6]


def unpack(total, stage, gram, extra=None):
    for p in range(64):
        stage[6 * p : 6 * p + 6] = total[p]
    side = stage[128:256]
    gram[:128, :128] = stage[:128]
    gram[:128, 128:] = side
    gram[128:, :128] = side.T
    gram[128:, 128:] = stage[256:]
    if extra is not None:
        extra[...] = stage[384 - NK :, :NK]
        lane = lax.broadcasted_iota(jnp.int32, (NK, 128), 1)
        turned = stage[256:].T[128 - NK :]
        gram[256 - NK :, 128:] = jnp.where(lane < NK, turned, stage[384 - NK :])


def inverse_factor(inner, size):
    groups = size // 8
    lane = lax.broadcasted_iota(jnp.int32, (8, size), 1)
    sub = lax.broadcasted_iota(jnp.int32, (8, size), 0)
    rest = [inner[8 * g : 8 * g + 8] for g in range(groups)]
    inv = [jnp.where(lane == sub + 8 * g, 1.0, 0.0).astype(F32) for g in range(groups)]

    def row(x, j):
        return jnp.broadcast_to(x[j : j + 1], (8, size))

    def column(x, j):
        return jnp.broadcast_to(x[:, j : j + 1], (8, size))

    diag = [column(rest[0], q) for q in range(8)]
    for b in range(groups):
        below = range(b + 1, groups)
        cols = {(j, g): column(rest[g], 8 * b + j) for g in below for j in range(8)}
        ahead = [column(rest[b + 1], 8 * b + 8 + q) for q in range(8)] if below else None
        roots = jnp.ones((8, size), F32)
        for j in range(8):
            root = lax.rsqrt(row(diag[j], j))
            scale = root * root
            roots = jnp.where(sub == j, root, roots)
            heads = {q: row(diag[q], j) for q in range(j + 1, 8)}
            rest_row, inv_row = row(rest[b], j), row(inv[b], j)
            step = jnp.where(sub > j, diag[j] * scale, 0.0)
            for q in heads:
                diag[q] = diag[q] - step * heads[q]
            rest[b] = rest[b] - step * rest_row
            inv[b] = inv[b] - step * inv_row
            for g in below:
                side = cols[j, g]
                step = side * scale
                for q in heads:
                    cols[q, g] = cols[q, g] - step * heads[q]
                rest[g] = rest[g] - step * rest_row
                inv[g] = inv[g] - step * inv_row
                if g == b + 1:
                    for q in range(8):
                        ahead[q] = ahead[q] - step * row(side, q)
        inv[b] = inv[b] * roots
        diag = ahead
    return jnp.concatenate(inv, axis=0) if groups > 1 else inv[0]


def advance(image, gram, going_on):
    lower = inverse_factor(full_dot(image, image, (1, 1)), image.shape[0])
    ahead = full_dot(image, gram)
    return full_dot(lower, jnp.where(going_on, ahead, image))


def orth(*pairs):
    for gram, basis in pairs:
        basis[...] = dot3(basis[...], gram[...])

    def step(i, c):
        values = [advance(basis[...], gram[...], i + 1 < ITERS) for gram, basis in pairs]
        for (_, basis), value in zip(pairs, values):
            basis[...] = value
        return c

    lax.fori_loop(0, ITERS, step, 0)


def swap(x):
    return pltpu.roll(x, 64, 1)


def regroup(a, b):
    left = lax.broadcasted_iota(jnp.int32, a.shape, 1) < 64
    return jnp.where(left, a, swap(b)), jnp.where(left, swap(a), b)


def main_kernel(
    x_hbm, start_f, start_s, start_r, start_c, rank_f, rank_s,
    xin, mixed_out, frames_out,
    xhi, xlo, acc, side, acc_s, gram, part_f, part_r, part_c,
    in_f, in_r, in_c, tot_f, tot_r, tot_c, stage, gram_s, bft, bst, brt, bct,
    red, kron_hi, kron_lo, back, send1, recv1, unf_hi, unf_lo, send2, recv2,
    load_sems, start_sems, sems, swap_sems,
):
    me = me_index()
    mine_row, mine_col = lax.axis_index("row"), lax.axis_index("col")
    for r in range(ROWS):
        pltpu.make_async_copy(x_hbm.at[r], xin.at[r], load_sems.at[r]).start()
    starts = [
        pltpu.make_async_copy(start, ref, start_sems.at[i])
        for i, (ref, start) in enumerate(((bft, start_f), (bst, start_s), (brt, start_r), (bct, start_c)))
    ]
    for copy in starts:
        copy.start()
    barrier = pltpu.get_barrier_semaphore()

    where = places()
    rows_of, cols_of = where[0], where[1]
    for dx, dy, dz, dk in PEERS:
        pl.semaphore_signal(barrier, inc=1, device_id=(rows_of[dx][dy], cols_of[dz][dk]), device_id_type=MESH)

    acc[...] = jnp.zeros_like(acc)
    side[...] = jnp.zeros_like(side)
    acc_s[...] = jnp.zeros_like(acc_s)
    def gather(r, c):
        pltpu.make_async_copy(x_hbm.at[r], xin.at[r], load_sems.at[r]).wait()
        hi, lo = halves(xin[r])
        xhi[r] = hi
        xlo[r] = lo
        acc[...] += dot(hi, hi, (0, 0))
        side[...] += dot(hi, lo, (0, 0))
        block = 0.0
        for q in range(0, LINES, 128):
            here = hi[q : q + 128]
            block += dot(here, jnp.concatenate([here, lo[q : q + 128]], axis=0), (1, 1))
        acc_s[...] += block
        return c

    lax.fori_loop(0, ROWS, gather, 0)
    mixed_in = acc_s[:, 128:]
    sends = acc_s[:, :128] + mixed_in + mixed_in.T
    j0 = lax.broadcasted_iota(jnp.int32, (128, 128), 0)
    j1 = lax.broadcasted_iota(jnp.int32, (128, 128), 1)
    sends = jnp.where(j0 // NK == j1 // NK, sends, 0.0).reshape(8, NK, 128).sum(axis=0)
    small = full_dot(sends, (j0 % NK == j1).astype(F32))
    pack(acc[...] + side[...] + side[...].T, part_f, small)

    for copy in starts:
        copy.wait()
    pl.semaphore_wait(barrier, NDEV - 1)
    finish_f = all_sum(where, part_f, in_f, tot_f, sems.at[0])

    unpack(tot_f, stage, gram, gram_s)

    orth((gram, bft), (gram_s, bst))
    keep_f = lax.broadcasted_iota(jnp.int32, (TMAX, NT), 0) < rank_f[0]
    frames_t = bft[...] * keep_f.astype(F32)
    frames_out[...] = frames_t
    keep_s = lax.broadcasted_iota(jnp.int32, (KMAX, NK), 0) < rank_s[0]
    sends = bst[...] * keep_s.astype(F32)
    a0 = lax.broadcasted_iota(jnp.int32, (KMAX, 256), 0)
    a1 = lax.broadcasted_iota(jnp.int32, (KMAX, 256), 1)
    wide = full_dot(sends, (a0 == a1 // COLS).astype(F32), (0, 0))
    c0 = lax.broadcasted_iota(jnp.int32, (LINES, 256), 0)
    c1 = lax.broadcasted_iota(jnp.int32, (LINES, 256), 1)
    spread = jnp.where(c0 // NK == c1 % COLS, jnp.concatenate([wide] * COLS, axis=0), 0.0)
    for part, value in zip((kron_hi, kron_lo), halves(spread)):
        part[0] = value[:, :128]
        part[1] = value[:, 128:]

    f_hi, f_lo = halves(frames_t)
    f_two = jnp.concatenate([f_hi, f_lo], axis=0)
    for r in range(ROWS):
        both_ways = dot(f_two, xhi[r], (1, 1))
        here = both_ways[:TMAX] + both_ways[TMAX:] + dot(f_hi, xlo[r], (1, 1))
        for q in range(4):
            red[q, pl.ds((r // 8) * 256 + r % 8, TMAX, stride=8), :] = here[:, 128 * q : 128 * q + 128]
    own = mine_col * 16 + mine_row
    parity = lax.rem(lax.div(mine_row, 4), 2)
    r_hi, r_lo = halves(jnp.concatenate([red[q] for q in range(4)], axis=1))
    for odd in range(2):
        t = 1 - parity if odd else parity
        twice = dot(r_hi, jnp.concatenate([kron_hi[t], kron_lo[t]], axis=1))
        core = twice[:, :128] + twice[:, 128:] + dot(r_lo, kron_hi[t])
        one, two = regroup(core[:256], core[256:])
        send1[pl.ds(32 * t, 32)] = one.reshape(32, 8, 128)
        send1[pl.ds(64 + 32 * t, 32)] = two.reshape(32, 8, 128)
        if not odd:
            recv1[own] = send1[me]
        for dx, dy, dz, dk in PEERS:
            if dx % 2 == odd:
                row, col = rows_of[dx][dy], cols_of[dz][dk]
                remote(send1.at[row * 8 + col], recv1.at[own], swap_sems.at[0], swap_sems.at[1], (row, col)).start()
    wait_for(recv1, NDEV - 1, swap_sems.at[1])

    for p in range(4):
        lanes = slice(128 * p, 128 * p + 128)
        one, two = regroup(
            recv1[32 * p : 32 * p + 16].reshape(128, 128), recv1[32 * p + 16 : 32 * p + 32].reshape(128, 128)
        )
        both_halves = [one.reshape(16, 1, 8, 128), two.reshape(16, 1, 8, 128)]
        unf_hi[:, lanes], unf_lo[:, lanes] = halves(jnp.concatenate(both_halves, axis=1).reshape(256, 128))
    pack(self_dot((unf_hi[...], unf_lo[...])), part_r)
    finish_r = all_sum(where, part_r, in_r, tot_r, sems.at[1])
    unpack(tot_r, stage, gram)
    orth((gram, brt))

    second = split_dot(halves(brt[...]), (unf_hi[...], unf_lo[...]))
    turned = second.T.reshape(8, 2, 32, RS)
    cols = [halves(turned[:, e].reshape(256, RS)) for e in range(2)]
    pack(self_dot(cols[0]) + self_dot(cols[1]), part_c)
    finish_c = all_sum(where, part_c, in_c, tot_c, sems.at[2])
    unpack(tot_c, stage, gram)
    orth((gram, bct))

    by_col, by_row = halves(bct[...].T), halves(brt[...].T)
    col_parts = halves(bct[...])
    backs = []
    for e in range(2):
        third = split_dot(col_parts, cols[e])
        backs.append(split_dot(by_col, halves(third)).reshape(8, 1, 32, RS))
    back[...] = jnp.concatenate(backs, axis=1).reshape(4, 128, RS)
    for near in (2, 1, 3, 0):
        p = where[2][near]
        pairs = split_dot(by_row, halves(back[p]), (1, 1)).reshape(16, 2, 8, 128)
        one, two = regroup(pairs[:, 0].reshape(128, 128), pairs[:, 1].reshape(128, 128))
        send2[pl.ds(32 * p, 16)] = one.reshape(16, 8, 128)
        send2[pl.ds(32 * p + 16, 16)] = two.reshape(16, 8, 128)
        if near == 0:
            recv2[me] = send2[own]
        for dx, dy, dz, dk in PEERS:
            if dz == near:
                row, col = rows_of[dx][dy], cols_of[dz][dk]
                remote(send2.at[col * 16 + row], recv2.at[me], swap_sems.at[2], swap_sems.at[3], (row, col)).start()
    wait_for(recv2, NDEV - 1, swap_sems.at[3])
    upper, lower = [], []
    for t in range(2):
        one, two = regroup(
            recv2[32 * t : 32 * t + 32].reshape(256, 128), recv2[64 + 32 * t : 96 + 32 * t].reshape(256, 128)
        )
        upper.append(one)
        lower.append(two)
    whole = jnp.concatenate([jnp.concatenate(upper, axis=1), jnp.concatenate(lower, axis=1)], axis=0)
    kron = [jnp.concatenate([part[0], part[1]], axis=1) for part in (kron_hi, kron_lo)]
    mixed = split_dot(halves(whole), kron, (1, 1))
    for q in range(4):
        mixed_out[q] = mixed[:, 128 * q : 128 * q + 128]
    for finish in (finish_f, finish_r, finish_c):
        finish()
    wait_for(send1, NDEV - 1, swap_sems.at[0])
    wait_for(send2, NDEV - 1, swap_sems.at[2])


def last_kernel(x_ref, mixed, frames, out_hbm, o_buf, store_sems):
    f_hi, f_lo = halves(frames[...])
    flat = jnp.concatenate([f_hi, f_hi, f_lo], axis=0)
    for r in range(ROWS):
        lines = pl.ds((r // 8) * 256 + r % 8, TMAX, stride=8)
        m_hi, m_lo = halves(jnp.concatenate([mixed[q, lines, :] for q in range(4)], axis=1))
        tall = jnp.concatenate([m_hi, m_lo, m_hi], axis=0)
        o_buf[r] = x_ref[r] - dot(tall, flat, (0, 0))
        pltpu.make_async_copy(o_buf.at[r], out_hbm.at[r], store_sems.at[r]).start()
    for r in range(ROWS):
        pltpu.make_async_copy(o_buf.at[r], out_hbm.at[r], store_sems.at[r]).wait()


def local(signal, start_frames, start_sends, start_rows, start_cols, rank_frames, rank_sends):
    x = signal.reshape(ROWS, LINES, NT)
    vmem = pl.BlockSpec(memory_space=pltpu.VMEM)
    smem = pl.BlockSpec(memory_space=pltpu.SMEM)
    hbm = pl.BlockSpec(memory_space=pltpu.HBM)
    tiles = lambda n: pltpu.VMEM((n, 8, 128), F32)
    flat = lambda *dims: pltpu.VMEM(dims, F32)
    short = lambda *dims: pltpu.VMEM(dims, BF16)
    held, mixed, frames = pl.pallas_call(
        main_kernel,
        out_shape=(pltpu.VMEM(x.shape, F32), pltpu.VMEM((4, 512, 128), F32), pltpu.VMEM((TMAX, NT), F32)),
        in_specs=[hbm, hbm, hbm, hbm, hbm, smem, smem],
        out_specs=(vmem, vmem, vmem),
        scratch_shapes=[
            pltpu.VMEM((ROWS, LINES, NT), BF16), pltpu.VMEM((ROWS, LINES, NT), BF16),
            flat(256, 256), flat(256, 256), flat(128, 256), flat(256, 256),
            flat(64, 6, 128), flat(64, 6, 128), flat(64, 6, 128),
            flat(NDEV - 1, 6, 128), flat(NDEV - 1, 6, 128), flat(NDEV - 1, 6, 128),
            flat(64, 6, 128), flat(64, 6, 128), flat(64, 6, 128), flat(384, 128), flat(NK, NK),
            flat(TMAX, NT), flat(KMAX, NK), flat(RS, 256), flat(RS, 256),
            flat(4, 512, 128), short(2, 512, 128), short(2, 512, 128), flat(4, 128, RS), tiles(NDEV), tiles(NDEV),
            short(256, 512), short(256, 512), tiles(NDEV), tiles(NDEV),
            pltpu.SemaphoreType.DMA((ROWS,)), pltpu.SemaphoreType.DMA((4,)), pltpu.SemaphoreType.DMA((3, 4)), pltpu.SemaphoreType.DMA((4,)),
        ],
        compiler_params=pltpu.CompilerParams(
            collective_id=1, has_side_effects=True, vmem_limit_bytes=57573376
        ),
        name="modes",
    )(x, start_frames.T, start_sends.T, start_rows.T, start_cols.T, rank_frames, rank_sends)
    out = pl.pallas_call(
        last_kernel,
        out_shape=jax.ShapeDtypeStruct(x.shape, F32),
        in_specs=[vmem, vmem, vmem],
        out_specs=pl.BlockSpec(memory_space=pl.ANY),
        scratch_shapes=[flat(ROWS, LINES, NT), pltpu.SemaphoreType.DMA((ROWS,))],
        compiler_params=pltpu.CompilerParams(vmem_limit_bytes=24 * 1024 * 1024),
        name="subtract",
    )(held, mixed, frames)
    return out.reshape(signal.shape)


def solution(mesh):
    return jax.shard_map(
        local,
        mesh=mesh,
        in_specs=(P("row", "col", None, None), P(), P(), P(), P(), P(), P()),
        out_specs=P("row", "col", None, None),
        check_vma=False,
    )
```
